8 devices in a mesh: dp: 1 (over z), sx: 2 (over y), sy: 4 (over x, core).
Axes of the slice: x: 2, y: 2, z: 1, core: 2. Of those that a mesh axis runs over, the one named last changes fastest.
Arguments:
- act_in: bfloat16 [12, 2048, 16, 256], P('dp', 'sy', 'sx')
- norm_first: bfloat16 [2, 256], replicated
- w_first: bfloat16 [3, 3, 256, 128], replicated
- w_short: bfloat16 [256, 128], replicated
- norm_rest: bfloat16 [6, 2, 128], replicated
- w_rest: bfloat16 [5, 3, 3, 128, 128], replicated
- bias_rest: bfloat16 [7, 128], replicated
- w_out: bfloat16 [3, 3, 128, 3], replicated
- bias_out: bfloat16 [3], replicated
Outputs:
- output: float32 [12, 2048, 16, 3], P('dp', 'sy', 'sx')
All inputs are finite; a program needn't handle non-finite values.
Results may differ from the reference program's by a relative error of at most 0.00841722.
Values are sent between devices in bfloat16 or wider.
A program may use at most 1 GiB of HBM per device.

```python
import math
import jax
import jax.numpy as jnp
from jax import lax

SAMPLES = 12
IMG_H = 2048
IMG_W = 16
IN_CH = 256
MID_CH = 128
OUT_CH = 3
GROUPS = 32
GN_EPS = 1e-6


def normal_weight(key, shape, fan_in):
    return (jax.random.normal(key, shape, jnp.float32) * fan_in ** -0.5).astype(jnp.bfloat16)


def norm_params(key, layer_count, chan_count):
    gain_key, shift_key = jax.random.split(key)
    gains = 1.0 + 0.25 * jax.random.normal(gain_key, (layer_count, chan_count), jnp.float32)
    shifts = 0.25 * jax.random.normal(shift_key, (layer_count, chan_count), jnp.float32)
    return jnp.stack([gains, shifts], axis=1).astype(jnp.bfloat16)


def setup_inputs(seed: int = 0, part: int = 0) -> dict:
    base_key = jax.random.key(seed)
    act_keys = jax.random.split(jax.random.fold_in(base_key, part), 6)
    weight_keys = jax.random.split(base_key, 8)
    wave_count = 3
    base_noise = jax.random.normal(act_keys[0], (SAMPLES, IMG_H, IMG_W, IN_CH), jnp.float32)
    wave_amp = jax.random.normal(act_keys[1], (SAMPLES, wave_count, 1, IN_CH), jnp.float32)
    row_freq = jax.random.uniform(act_keys[2], (SAMPLES, wave_count, 1, 1), jnp.float32, 0.5, 2.5)
    col_freq = jax.random.uniform(act_keys[3], (SAMPLES, wave_count, 1, 1), jnp.float32, 0.5, 2.5)
    row_phase = jax.random.uniform(act_keys[4], (SAMPLES, wave_count, 1, IN_CH), jnp.float32, 0.0, 2.0 * math.pi)
    col_phase = jax.random.uniform(act_keys[5], (SAMPLES, wave_count, 1, IN_CH), jnp.float32, 0.0, 2.0 * math.pi)
    row_pos = (jnp.arange(IMG_H, dtype=jnp.float32) / IMG_H)[:, None]
    col_pos = (jnp.arange(IMG_W, dtype=jnp.float32) / IMG_W)[:, None]
    row_wave = wave_amp * jnp.cos(2.0 * math.pi * row_freq * row_pos + row_phase)
    col_wave = jnp.cos(2.0 * math.pi * col_freq * col_pos + col_phase)
    smooth_field = jnp.einsum("skhc,skwc->shwc", row_wave, col_wave)
    act_in = (0.7 * base_noise + smooth_field).astype(jnp.bfloat16)
    return {
        "act_in": act_in,
        "norm_first": norm_params(weight_keys[0], 1, IN_CH)[0],
        "w_first": normal_weight(weight_keys[1], (3, 3, IN_CH, MID_CH), 9 * IN_CH),
        "w_short": normal_weight(weight_keys[2], (IN_CH, MID_CH), IN_CH),
        "norm_rest": norm_params(weight_keys[3], 6, MID_CH),
        "w_rest": normal_weight(weight_keys[4], (5, 3, 3, MID_CH, MID_CH), 9 * MID_CH),
        "bias_rest": (0.3 * jax.random.normal(weight_keys[5], (7, MID_CH), jnp.float32)).astype(jnp.bfloat16),
        "w_out": normal_weight(weight_keys[6], (3, 3, MID_CH, OUT_CH), 9 * MID_CH),
        "bias_out": (0.3 * jax.random.normal(weight_keys[7], (OUT_CH,), jnp.float32)).astype(jnp.bfloat16),
    }


def group_norm_act(act_map, norm_pair):
    num_rows, num_cols, channels = act_map.shape
    per_group = channels // GROUPS
    group_count = num_rows * num_cols * per_group
    sum_one = jnp.sum(act_map, axis=(0, 1), dtype=jnp.float32).reshape(GROUPS, per_group).sum(axis=1)
    sum_two = jnp.sum(jnp.square(act_map.astype(jnp.float32)), axis=(0, 1)).reshape(GROUPS, per_group).sum(axis=1)
    group_mean = sum_one / group_count
    inv_std = lax.rsqrt(sum_two / group_count - group_mean * group_mean + GN_EPS)
    chan_scale = jnp.repeat(inv_std, per_group) * norm_pair[0].astype(jnp.float32)
    chan_shift = norm_pair[1].astype(jnp.float32) - jnp.repeat(group_mean, per_group) * chan_scale
    return jax.nn.silu(act_map.astype(jnp.float32) * chan_scale + chan_shift).astype(jnp.bfloat16)


def conv_three(act_map, kernel):
    num_rows, num_cols, in_chans = act_map.shape
    padded = jnp.pad(act_map, ((1, 1), (1, 1), (0, 0)))
    accum_sum = jnp.zeros((num_rows * num_cols, kernel.shape[3]), jnp.float32)
    for row_off in range(3):
        for col_off in range(3):
            window = padded[row_off:row_off + num_rows, col_off:col_off + num_cols].reshape(num_rows * num_cols, in_chans)
            accum_sum = accum_sum + jnp.dot(window, kernel[row_off, col_off], preferred_element_type=jnp.float32)
    return accum_sum.reshape(num_rows, num_cols, kernel.shape[3])


def reference(act_in, norm_first, w_first, w_short, norm_rest, w_rest, bias_rest, w_out, bias_out):
    bias_rows = bias_rest.astype(jnp.float32)

    def decode_sample(sample):
        num_rows, num_cols, in_chans = sample.shape
        mid_act = (conv_three(group_norm_act(sample, norm_first), w_first) + bias_rows[0]).astype(jnp.bfloat16)
        skip_path = jnp.dot(sample.reshape(num_rows * num_cols, in_chans), w_short, preferred_element_type=jnp.float32).reshape(num_rows, num_cols, -1) + bias_rows[6]
        hidden = (conv_three(group_norm_act(mid_act, norm_rest[0]), w_rest[0]) + bias_rows[1] + skip_path).astype(jnp.bfloat16)
        for res_index in range(1, 3):
            first_at = 2 * res_index - 1
            mid_act = (conv_three(group_norm_act(hidden, norm_rest[first_at]), w_rest[first_at]) + bias_rows[first_at + 1]).astype(jnp.bfloat16)
            hidden = (conv_three(group_norm_act(mid_act, norm_rest[first_at + 1]), w_rest[first_at + 1]) + bias_rows[first_at + 2] + hidden.astype(jnp.float32)).astype(jnp.bfloat16)
        return conv_three(group_norm_act(hidden, norm_rest[5]), w_out) + bias_out.astype(jnp.float32)

    return lax.map(decode_sample, act_in)
```

```python
import functools

import jax
import jax.numpy as jnp
from jax import lax
from jax.experimental import pallas as pl
from jax.experimental.pallas import tpu as pltpu
from jax.sharding import PartitionSpec as P

GROUPS = 32
GN_EPS = 1e-6
LANES = 128
SEGS = 16
MESH = pl.DeviceIdType.MESH
F32 = jnp.float32
BF16 = jnp.bfloat16


def decode_kernel(cfg, a_hbm, nf_ref, wf_hbm, ws_hbm, nr_ref, wr_hbm, br_ref, wo_ref, bo_ref, out_ref,
                  wide, thin, act, w_one, w_two, w_mid, halo_even, halo_odd, land, shuffle, bias_f,
                  row_send, row_recv, cor_send, cor_recv, stat,
                  land_sem, w_sem, col_ss, col_rs, row_ss, row_rs, cor_ss, cor_rs, stat_ss, stat_rs):
    samples, segrows, cols, n_sx, n_sy = cfg
    devices = n_sx * n_sy
    px = segrows * SEGS
    sx = lax.axis_index("sx")
    sy = lax.axis_index("sy")
    me = sx * n_sy + sy
    edge = (cols - 1) * (1 - sx)
    pixels = segrows * SEGS * cols * devices

    barrier = pltpu.get_barrier_semaphore()
    peers = []
    for k in range(1, devices):
        peers.append({"sx": lax.rem(sx + k // n_sy, n_sx), "sy": lax.rem(sy + k % n_sy, n_sy)})
    for peer in peers:
        pl.semaphore_signal(barrier, inc=1, device_id=peer, device_id_type=MESH)

    def land_copy(i, slot):
        return pltpu.make_async_copy(a_hbm.at[i], land.at[slot], land_sem.at[slot])

    land_copy(0, 0).start()

    weight_copies = []
    for e in range(2):
        lanes = pl.ds(e * LANES, LANES)
        for dr in range(3):
            weight_copies.append((wf_hbm.at[dr], w_one.at[dr, pl.ds(e, 3), :, lanes]))
            weight_copies.append((wr_hbm.at[0, dr], w_two.at[dr, pl.ds(e, 3), :, lanes]))
            for layer in range(4):
                weight_copies.append((wr_hbm.at[layer + 1, dr], w_mid.at[layer, dr, pl.ds(e, 3), :, lanes]))
        for half in range(2):
            weight_copies.append((ws_hbm.at[pl.ds(half * LANES, LANES)], w_two.at[3, 2 * e + half, :, lanes]))
    weight_copies = [pltpu.make_async_copy(src, dst, w_sem.at[n]) for n, (src, dst) in enumerate(weight_copies)]
    for copy in weight_copies:
        copy.start()
    zero_one = jnp.zeros((2 * LANES, LANES), BF16)
    zero_block = jnp.zeros((LANES, LANES), BF16)
    for e in range(2):
        lanes = slice(e * LANES, (e + 1) * LANES)
        for dr in range(3):
            w_one[dr, 3 - 3 * e, :, lanes] = zero_one
            w_two[dr, 3 - 3 * e, :, lanes] = zero_block
            for layer in range(4):
                w_mid[layer, dr, 3 - 3 * e, :, lanes] = zero_block
        for half in range(2):
            w_two[3, 2 * (1 - e) + half, :, lanes] = zero_block
    bias_f[...] = br_ref[...].astype(F32)
    zero_col = (cols + 1) * sx
    for half in range(2):
        act[half, zero_col] = jnp.zeros((segrows + 2, SEGS, LANES), BF16)

    pl.semaphore_wait(barrier, devices - 1)

    def copies(par, first, i):
        found = []
        if first:
            col_src, col_dst = wide.at[i, :, edge], halo_even.at[i]
        elif par == 0:
            col_src, col_dst = wide.at[i, 0, edge], halo_even.at[i, 0]
        else:
            col_src, col_dst = thin.at[i, edge], halo_odd.at[i]
        pick = (lambda ref: ref) if first else (lambda ref: ref.at[0])
        mine = pick(stat.at[par, i, me])
        for k, peer in enumerate(peers):
            found.append((mine, mine, stat_ss.at[par, i, k], stat_rs.at[par, i, k], peer))
        for t in range(2):
            other = lax.rem(sy + (n_sy - 1 if t == 0 else 1), n_sy)
            found.append((pick(row_send.at[i, t]), pick(row_recv.at[par, i, 1 - t]), row_ss.at[par, i, t], row_rs.at[par, i, t], {"sx": sx, "sy": other}))
            found.append((pick(cor_send.at[i, t]), pick(cor_recv.at[par, i, 1 - t]), cor_ss.at[par, i, t], cor_rs.at[par, i, t], {"sx": 1 - sx, "sy": other}))
        found.append((col_src, col_dst, col_ss.at[par, i], col_rs.at[par, i], {"sx": 1 - sx, "sy": sy}))
        return [
            pltpu.make_async_remote_copy(src_ref=src, dst_ref=dst, send_sem=ss, recv_sem=rs, device_id=peer, device_id_type=MESH)
            for src, dst, ss, rs, peer in found
        ]

    def send(par, first, i, sums):
        buf = wide if par == 0 else thin
        for half in range(2 if first else 1):
            stat[par, i, me, half] = jnp.concatenate([jnp.sum(part, axis=0, keepdims=True) for part in sums[half]], axis=0)
            for t in range(2):
                for c in range(cols):
                    where = (i, half, c) if par == 0 else (i, c)
                    tile = buf[where + (t * (segrows - 1),)].astype(F32)
                    row_send[i, t, half, pl.ds(c, 1), :] = tile[t * (SEGS - 1):t * (SEGS - 1) + 1]
                cor_send[i, t, half] = row_send[i, t, half, pl.ds(edge, 1), :]
        for copy in copies(par, first, i):
            copy.start()

    def prepare(i, _):
        slot = lax.rem(i, 2)
        land_copy(i, slot).wait()

        @pl.when(i + 1 < samples)
        def _():
            land_copy(i + 1, 1 - slot).start()

        def relayout(r, sums):
            new = []
            for half in range(2):
                block = land[slot, :, r, :, pl.ds(half * LANES, LANES)].astype(F32)
                s_one, s_two = sums[half]
                new.append((s_one + jnp.sum(block, axis=0), s_two + jnp.sum(block * block, axis=0)))
                shuffle[half] = block.reshape(SEGS * cols, LANES)
                for c in range(cols):
                    wide[i, half, c, r] = shuffle[half, pl.ds(c, SEGS, stride=cols), :].astype(BF16)
            return tuple(new)

        zero = jnp.zeros((8, LANES), F32)
        sums = lax.fori_loop(0, segrows, relayout, ((zero, zero), (zero, zero)))
        send(0, True, i, sums)
        return 0

    lax.fori_loop(0, samples, prepare, 0)
    for copy in weight_copies:
        copy.wait()

    lane = lax.broadcasted_iota(jnp.int32, (2, LANES), 1)
    seg_at = lax.broadcasted_iota(jnp.int32, (SEGS, LANES), 0)

    def group_total(x, size):
        step = 1
        while step < size:
            x = x + jnp.where((lane & step) != 0, pltpu.roll(x, step, 1), pltpu.roll(x, LANES - step, 1))
            step *= 2
        return x

    def silu_half(x, scale, shift):
        v = x * scale + shift
        return v + v * jnp.tanh(v)

    def activate(par, first, i, pair_of):
        for copy in copies(par, first, i):
            copy.wait()
        per_group = (2 if first else 1) * LANES // GROUPS
        count = pixels * per_group
        for half in range(2 if first else 1):
            total = stat[par, i, 0, half]
            for dev in range(1, devices):
                total = total + stat[par, i, dev, half]
            total = group_total(total, per_group) * (1.0 / count)
            mean, square = total[0:1], total[1:2]
            gamma, beta = pair_of(half)
            scale = gamma * lax.rsqrt(square - mean * mean + GN_EPS)
            shift = beta - mean * scale
            scale, shift = 0.5 * scale, 0.5 * shift

            def column(src, above, below, dst):
                z = silu_half(src.astype(F32), scale, shift)
                act[half, dst, 1:segrows + 1] = z.astype(BF16)
                above = jnp.where(sy > 0, silu_half(above, scale, shift), 0.0)
                below = jnp.where(sy < n_sy - 1, silu_half(below, scale, shift), 0.0)
                act[half, dst, 0] = jnp.where(seg_at == 0, above, pltpu.roll(z[segrows - 1], 1, 0)).astype(BF16)
                act[half, dst, segrows + 1] = jnp.where(seg_at == SEGS - 1, below, pltpu.roll(z[0], SEGS - 1, 0)).astype(BF16)

            def own(c, _):
                src = wide[i, half, c] if par == 0 else thin[i, c]
                column(src, row_recv[par, i, 0, half, pl.ds(c, 1), :], row_recv[par, i, 1, half, pl.ds(c, 1), :], c + 1)
                return 0

            lax.fori_loop(0, cols, own, 0)
            src = halo_even[i, half] if par == 0 else halo_odd[i]
            column(src, cor_recv[par, i, 0, half], cor_recv[par, i, 1, half], (cols + 1) * (1 - sx))

    def conv(par, first, i, weights, bias, skip, residual):
        halves = 2 if first else 1

        def pair(p, sums):
            pieces = []
            for dr in range(3):
                for j in range(4):
                    for half in range(halves):
                        pieces.append(act[half, 2 * p + j, dr:dr + segrows].reshape(px, LANES))
            if skip:
                for e in range(2):
                    for half in range(2):
                        pieces.append(wide[i, half, 2 * p + e].reshape(px, LANES))
            res = jnp.dot(jnp.concatenate(pieces, axis=1), weights(), preferred_element_type=F32)
            s_one, s_two = sums
            for e in range(2):
                y = res[:, e * LANES:(e + 1) * LANES] + bias
                if residual:
                    y = y + wide[i, 0, 2 * p + e].reshape(px, LANES).astype(F32)
                rounded = y.astype(BF16)
                if par == 0:
                    thin[i, 2 * p + e] = rounded.reshape(segrows, SEGS, LANES)
                else:
                    wide[i, 0, 2 * p + e] = rounded.reshape(segrows, SEGS, LANES)
                back = rounded.astype(F32).reshape(px // 8, 8, LANES)
                s_one = s_one + jnp.sum(back, axis=0)
                s_two = s_two + jnp.sum(back * back, axis=0)
            return s_one, s_two

        zero = jnp.zeros((8, LANES), F32)
        sums = lax.fori_loop(0, cols // 2, pair, (zero, zero))
        send(1 - par, False, i, [sums])

    def rest_pair(at):
        pair = nr_ref[at].astype(F32)
        return lambda half: (pair[0:1], pair[1:2])

    def first_pair(half):
        pair = nf_ref[:, half * LANES:(half + 1) * LANES].astype(F32)
        return pair[0:1], pair[1:2]

    def layer_one(i, _):
        activate(0, True, i, first_pair)
        conv(0, True, i, lambda: w_one[...].reshape(24 * LANES, 2 * LANES), bias_f[0:1], False, False)
        return 0

    def layer_two(i, _):
        activate(1, False, i, rest_pair(0))
        conv(1, False, i, lambda: w_two[...].reshape(16 * LANES, 2 * LANES), bias_f[1:2] + bias_f[6:7], True, False)
        return 0

    lax.fori_loop(0, samples, layer_one, 0)
    lax.fori_loop(0, samples, layer_two, 0)

    def block(k, _):
        def body(which):
            def layer(i, _):
                at = 2 * k + which
                activate(which, False, i, rest_pair(at + 1))
                conv(which, False, i, lambda: w_mid[at].reshape(12 * LANES, 2 * LANES), bias_f[pl.ds(at + 2, 1), :], False, which == 1)
                return 0
            return layer

        lax.fori_loop(0, samples, body(0), 0)
        lax.fori_loop(0, samples, body(1), 0)
        return 0

    lax.fori_loop(0, 2, block, 0)

    def head(i, _):
        activate(0, False, i, rest_pair(5))

        def column(c, _):
            pieces = []
            for dr in range(3):
                for dc in range(3):
                    pieces.append(act[0, c + dc, dr:dr + segrows].reshape(px, LANES))
            y = lax.dot_general(wo_ref[...], jnp.concatenate(pieces, axis=1), (((1,), (1,)), ((), ())), preferred_element_type=F32)
            for ch in range(3):
                out_ref[i, ch, pl.ds(c, 1), :] = y[ch:ch + 1] + bo_ref[ch:ch + 1, 0:1]
            return 0

        lax.fori_loop(0, cols, column, 0)
        return 0

    lax.fori_loop(0, samples, head, 0)


def solution(mesh):
    n_sy = mesh.shape["sy"]
    n_sx = mesh.shape["sx"]
    devices = n_sx * n_sy
    tile_spec = P("dp", "sy", "sx", None)
    replicated = P()

    def local_decode(act_in, norm_first, w_first, w_short, norm_rest, w_rest, bias_rest, w_out, bias_out):
        samples, rows, cols, chans = act_in.shape
        segrows = rows // SEGS
        act_five = act_in.reshape(samples, SEGS, segrows, cols, chans)
        head_w = jnp.pad(jnp.transpose(w_out, (3, 0, 1, 2)).reshape(3, 9 * LANES), ((0, 13), (0, 0)))
        head_b = jnp.broadcast_to(jnp.pad(bias_out.astype(F32), (0, 5))[:, None], (8, LANES))
        vmem = pl.BlockSpec(memory_space=pltpu.VMEM)
        hbm = pl.BlockSpec(memory_space=pl.ANY)
        dma = pltpu.SemaphoreType.DMA
        scratch = [
            pltpu.VMEM((samples, 2, cols, segrows, SEGS, LANES), BF16),
            pltpu.VMEM((samples, cols, segrows, SEGS, LANES), BF16),
            pltpu.VMEM((2, cols + 2, segrows + 2, SEGS, LANES), BF16),
            pltpu.VMEM((3, 4, 2 * LANES, 2 * LANES), BF16),
            pltpu.VMEM((4, 4, LANES, 2 * LANES), BF16),
            pltpu.VMEM((4, 3, 4, LANES, 2 * LANES), BF16),
            pltpu.VMEM((samples, 2, segrows, SEGS, LANES), BF16),
            pltpu.VMEM((samples, segrows, SEGS, LANES), BF16),
            pltpu.VMEM((2, SEGS, segrows, cols, chans), BF16),
            pltpu.VMEM((2, SEGS * cols, LANES), F32),
            pltpu.VMEM((7, LANES), F32),
            pltpu.VMEM((samples, 2, 2, cols, LANES), F32),
            pltpu.VMEM((2, samples, 2, 2, cols, LANES), F32),
            pltpu.VMEM((samples, 2, 2, 1, LANES), F32),
            pltpu.VMEM((2, samples, 2, 2, 1, LANES), F32),
            pltpu.VMEM((2, samples, devices, 2, 2, LANES), F32),
            dma((2,)),
            dma((40,)),
            dma((2, samples)),
            dma((2, samples)),
            dma((2, samples, 2)),
            dma((2, samples, 2)),
            dma((2, samples, 2)),
            dma((2, samples, 2)),
            dma((2, samples, devices - 1)),
            dma((2, samples, devices - 1)),
        ]
        cfg = (samples, segrows, cols, n_sx, n_sy)
        image = pl.pallas_call(
            functools.partial(decode_kernel, cfg),
            out_shape=jax.ShapeDtypeStruct((samples, 3, cols, rows), F32),
            in_specs=[hbm, vmem, hbm, hbm, vmem, hbm, vmem, vmem, vmem],
            out_specs=vmem,
            scratch_shapes=scratch,
            compiler_params=pltpu.CompilerParams(collective_id=0, has_side_effects=True, vmem_limit_bytes=67043328),
        )(act_five, norm_first, w_first, w_short, norm_rest, w_rest, bias_rest, head_w, head_b)
        image = image.reshape(samples, 3, cols, segrows, SEGS)
        return jnp.transpose(image, (0, 4, 3, 2, 1)).reshape(samples, rows, cols, 3)

    return jax.shard_map(local_decode, mesh=mesh, in_specs=(tile_spec, replicated, replicated, replicated, replicated, replicated, replicated, replicated, replicated), out_specs=tile_spec, check_vma=False)
```

```python
import functools

import jax
import jax.numpy as jnp
from jax import lax
from jax.experimental import pallas as pl
from jax.experimental.pallas import tpu as pltpu
from jax.sharding import PartitionSpec as P

GROUPS = 32
GN_EPS = 1e-6
LANES = 128
SEGS = 16
MESH = pl.DeviceIdType.MESH
F32 = jnp.float32
BF16 = jnp.bfloat16


def decode_kernel(cfg, a_hbm, nf_ref, wf_hbm, ws_hbm, nr_ref, wr_hbm, br_ref, wo_ref, bo_ref, out_ref,
                  wide, thin, act_a, act_b, w_one, w_two, w_mid, halo_even, halo_odd, land, shuffle, bias_f,
                  row_send, row_recv, cor_send, cor_recv, stat, tally, head_f, head_w, order, part, image, q_send, q_recv,
                  land_sem, w_sem, col_ss, col_rs, small_ss, small_rs, q_ss, q_rs):
    samples, segrows, cols, n_sx, n_sy = cfg
    devices = n_sx * n_sy
    px = segrows * SEGS
    sx = lax.axis_index("sx")
    sy = lax.axis_index("sy")
    me = sx * n_sy + sy
    edge = (cols - 1) * (1 - sx)
    pixels = segrows * SEGS * cols * devices
    acts = (act_a, act_b)

    barrier = pltpu.get_barrier_semaphore()
    peers = []
    for k in range(1, devices):
        peers.append({"sx": lax.rem(sx + k // n_sy, n_sx), "sy": lax.rem(sy + k % n_sy, n_sy)})
    for peer in peers:
        pl.semaphore_signal(barrier, inc=1, device_id=peer, device_id_type=MESH)

    def land_copy(i, slot):
        return pltpu.make_async_copy(a_hbm.at[i], land.at[slot], land_sem.at[slot])

    land_copy(0, 0).start()

    weight_copies = []
    for e in range(2):
        lanes = pl.ds(e * LANES, LANES)
        for dr in range(3):
            weight_copies.append((wf_hbm.at[dr], w_one.at[dr, pl.ds(e, 3), :, lanes]))
            weight_copies.append((wr_hbm.at[0, dr], w_two.at[dr, pl.ds(e, 3), :, lanes]))
            for layer in range(4):
                weight_copies.append((wr_hbm.at[layer + 1, dr], w_mid.at[layer, dr, pl.ds(e, 3), :, lanes]))
        for half in range(2):
            weight_copies.append((ws_hbm.at[pl.ds(half * LANES, LANES)], w_two.at[3, 2 * e + half, :, lanes]))
    weight_copies = [pltpu.make_async_copy(src, dst, w_sem.at[n]) for n, (src, dst) in enumerate(weight_copies)]

    pl.semaphore_wait(barrier, devices - 1)

    def column_copy(par, first, i):
        if first:
            src, dst = wide.at[i, :, edge], halo_even.at[i]
        elif par == 0:
            src, dst = wide.at[i, 0, edge], halo_even.at[i, 0]
        else:
            src, dst = thin.at[i, edge], halo_odd.at[i]
        return pltpu.make_async_remote_copy(
            src_ref=src, dst_ref=dst, send_sem=col_ss.at[par, i], recv_sem=col_rs.at[par, i],
            device_id={"sx": 1 - sx, "sy": sy}, device_id_type=MESH)

    def small_copies(par, first, i):
        pick = (lambda ref: ref) if first else (lambda ref: ref.at[0])
        mine = pick(stat.at[par, i, me])
        found = [(mine, mine, peer) for peer in peers]
        for t in range(2):
            other = lax.rem(sy + (n_sy - 1 if t == 0 else 1), n_sy)
            found.append((pick(row_send.at[i, t]), pick(row_recv.at[par, i, 1 - t]), {"sx": sx, "sy": other}))
            found.append((pick(cor_send.at[i, t]), pick(cor_recv.at[par, i, 1 - t]), {"sx": 1 - sx, "sy": other}))
        return [
            pltpu.make_async_remote_copy(src_ref=src, dst_ref=dst, send_sem=small_ss.at[par, i], recv_sem=small_rs.at[par, i], device_id=peer, device_id_type=MESH)
            for src, dst, peer in found
        ]

    def await_copies(par, first, i, with_column):
        size = tally if first else tally.at[0]
        pltpu.make_async_copy(size, size, small_ss.at[par, i]).wait()
        pltpu.make_async_copy(size, size, small_rs.at[par, i]).wait()
        if with_column:
            column_copy(par, first, i).wait()

    def send(par, first, i, sums, with_column):
        buf = wide if par == 0 else thin
        for half in range(2 if first else 1):
            stat[par, i, me, half] = jnp.concatenate([jnp.sum(part_sum, axis=0, keepdims=True) for part_sum in sums[half]], axis=0)
            for t in range(2):
                for c in range(cols):
                    at = (i, half, c) if par == 0 else (i, c)
                    tile = buf[at + (t * (segrows - 1),)].astype(F32)
                    row_send[i, t, half, pl.ds(c, 1), :] = tile[t * (SEGS - 1):t * (SEGS - 1) + 1]
                cor_send[i, t, half] = row_send[i, t, half, pl.ds(edge, 1), :]
        for copy in small_copies(par, first, i):
            copy.start()
        if with_column:
            column_copy(par, first, i).start()

    def prepare(i, _):
        slot = lax.rem(i, 2)
        land_copy(i, slot).wait()

        @pl.when(i + 1 < samples)
        def _():
            land_copy(i + 1, 1 - slot).start()

        def relayout(r, sums):
            new = []
            for half in range(2):
                block = land[slot, :, r, :, pl.ds(half * LANES, LANES)].astype(F32)
                s_one, s_two = sums[half]
                new.append((s_one + jnp.sum(block, axis=0), s_two + jnp.sum(block * block, axis=0)))
                shuffle[half] = block.reshape(SEGS * cols, LANES)
                for c in range(cols):
                    wide[i, half, c, r] = shuffle[half, pl.ds(c, SEGS, stride=cols), :].astype(BF16)
            return tuple(new)

        zero = jnp.zeros((8, LANES), F32)
        sums = lax.fori_loop(0, segrows, relayout, ((zero, zero), (zero, zero)))
        send(0, True, i, sums, True)
        return 0

    prepare(0, 0)
    for copy in weight_copies:
        copy.start()
    zero_one = jnp.zeros((2 * LANES, LANES), BF16)
    zero_block = jnp.zeros((LANES, LANES), BF16)
    for e in range(2):
        lanes = slice(e * LANES, (e + 1) * LANES)
        for dr in range(3):
            w_one[dr, 3 - 3 * e, :, lanes] = zero_one
            w_two[dr, 3 - 3 * e, :, lanes] = zero_block
            for layer in range(4):
                w_mid[layer, dr, 3 - 3 * e, :, lanes] = zero_block
        for half in range(2):
            w_two[3, 2 * (1 - e) + half, :, lanes] = zero_block
    bias_f[...] = br_ref[...].astype(F32)
    zero_col = (cols + 1) * sx
    for half in range(2):
        for buf in acts:
            buf[half, zero_col] = jnp.zeros((segrows + 2, SEGS, LANES), BF16)
    head_f[...] = jnp.zeros(head_f.shape, F32)
    for dr in range(3):
        for kc in range(3):
            head_f[kc * 8:kc * 8 + 3, dr * LANES:(dr + 1) * LANES] = wo_ref[dr, kc].astype(F32)
    head_w[...] = head_f[...].astype(BF16)
    came = lax.broadcasted_iota(jnp.int32, (px, px), 0)
    goes = lax.broadcasted_iota(jnp.int32, (px, px), 1)
    order[...] = jnp.where(goes == lax.rem(came, SEGS) * segrows + lax.div(came, SEGS), 1.0, 0.0).astype(BF16)
    part[0, 0] = jnp.zeros((8, px), F32)
    part[cols + 1, 2] = jnp.zeros((8, px), F32)

    lax.fori_loop(1, samples, prepare, 0)
    for copy in weight_copies:
        copy.wait()

    lane = lax.broadcasted_iota(jnp.int32, (2, LANES), 1)
    seg_at = lax.broadcasted_iota(jnp.int32, (SEGS, LANES), 0)

    def group_total(x, size):
        step = 1
        while step < size:
            x = x + jnp.where((lane & step) != 0, pltpu.roll(x, step, 1), pltpu.roll(x, LANES - step, 1))
            step *= 2
        return x

    def silu_half(x, scale, shift):
        v = x * scale + shift
        return v + v * jnp.tanh(v)

    def norms(par, first, i, pair_of):
        per_group = (2 if first else 1) * LANES // GROUPS
        count = pixels * per_group
        found = []
        for half in range(2 if first else 1):
            total = stat[par, i, 0, half]
            for dev in range(1, devices):
                total = total + stat[par, i, dev, half]
            total = group_total(total, per_group) * (1.0 / count)
            mean, square = total[0:1], total[1:2]
            gamma, beta = pair_of(half)
            scale = gamma * lax.rsqrt(square - mean * mean + GN_EPS)
            shift = beta - mean * scale
            found.append((0.5 * scale, 0.5 * shift))
        return found

    def column(src, above, below, dst, scale, shift):
        z = silu_half(src.astype(F32), scale, shift)
        dst[1:segrows + 1] = z.astype(BF16)
        above = jnp.where(sy > 0, silu_half(above, scale, shift), 0.0)
        below = jnp.where(sy < n_sy - 1, silu_half(below, scale, shift), 0.0)
        dst[0] = jnp.where(seg_at == 0, above, pltpu.roll(z[segrows - 1], 1, 0)).astype(BF16)
        dst[segrows + 1] = jnp.where(seg_at == SEGS - 1, below, pltpu.roll(z[0], SEGS - 1, 0)).astype(BF16)

    def own_column(par, i, half, c, dst, scale, shift):
        src = wide[i, half, c] if par == 0 else thin[i, c]
        column(src, row_recv[par, i, 0, half, pl.ds(c, 1), :], row_recv[par, i, 1, half, pl.ds(c, 1), :], dst, scale, shift)

    def halo_column(par, first, i, buf, factors):
        for half, (scale, shift) in enumerate(factors):
            src = halo_even[i, half] if par == 0 else halo_odd[i]
            column(src, cor_recv[par, i, 0, half], cor_recv[par, i, 1, half], buf.at[half, (cols + 1) * (1 - sx)], scale, shift)

    def run_layer(par, first, pair_of, weights, bias, skip, residual, last, after):
        halves = 2 if first else 1

        await_copies(par, first, 0, True)
        start = norms(par, first, 0, pair_of)
        halo_column(par, first, 0, act_a, start)

        def own(c, _):
            for half, (scale, shift) in enumerate(start):
                own_column(par, 0, half, c, act_a.at[half, c + 1], scale, shift)
            return 0

        lax.fori_loop(0, cols, own, 0)

        def step(i, s):
            now, later = acts[s], acts[1 - s]
            if s == 0:
                ahead = i + 1
                await_copies(par, first, ahead, True)
            else:
                ahead = jnp.minimum(i + 1, samples - 1)

                @pl.when(i + 1 < samples)
                def _():
                    await_copies(par, first, ahead, True)

            factors = norms(par, first, ahead, pair_of)
            halo_column(par, first, ahead, later, factors)

            def pair(p, sums):
                pieces = []
                for dr in range(3):
                    for j in range(4):
                        for half in range(halves):
                            pieces.append(now[half, 2 * p + j, dr:dr + segrows].reshape(px, LANES))
                if skip:
                    for e in range(2):
                        for half in range(2):
                            pieces.append(wide[i, half, 2 * p + e].reshape(px, LANES))
                res = jnp.dot(jnp.concatenate(pieces, axis=1), weights(), preferred_element_type=F32)
                for half, (scale, shift) in enumerate(factors):
                    for e in range(2):
                        own_column(par, ahead, half, 2 * p + e, later.at[half, 2 * p + e + 1], scale, shift)
                s_one, s_two = sums
                for e in range(2):
                    y = res[:, e * LANES:(e + 1) * LANES] + bias
                    if residual:
                        y = y + wide[i, 0, 2 * p + e].reshape(px, LANES).astype(F32)
                    rounded = y.astype(BF16)
                    if par == 0:
                        thin[i, 2 * p + e] = rounded.reshape(segrows, SEGS, LANES)
                    else:
                        wide[i, 0, 2 * p + e] = rounded.reshape(segrows, SEGS, LANES)
                    back = rounded.astype(F32).reshape(px // 8, 8, LANES)
                    s_one = s_one + jnp.sum(back, axis=0)
                    s_two = s_two + jnp.sum(back * back, axis=0)
                return s_one, s_two

            zero = jnp.zeros((8, LANES), F32)
            sums = lax.fori_loop(0, cols // 2, pair, (zero, zero))
            send(1 - par, False, i, [sums], not last)
            after(i)

        def two(t, _):
            step(2 * t, 0)
            step(2 * t + 1, 1)
            return 0

        lax.fori_loop(0, samples // 2, two, 0)

    def rest_pair(at):
        def pair_of(half):
            pair = nr_ref[at].astype(F32)
            return pair[0:1], pair[1:2]
        return pair_of

    def first_pair(half):
        pair = nf_ref[:, half * LANES:(half + 1) * LANES].astype(F32)
        return pair[0:1], pair[1:2]

    def edge_copy(i):
        return pltpu.make_async_remote_copy(
            src_ref=q_send.at[i], dst_ref=q_recv.at[i], send_sem=q_ss.at[i], recv_sem=q_rs.at[i],
            device_id={"sx": 1 - sx, "sy": sy}, device_id_type=MESH)

    def head_products(i):
        await_copies(0, False, i, False)
        (scale, shift), = norms(0, False, i, rest_pair(5))
        buf = act_b.at[1]

        def column_product(c, _):
            own_column(0, i, 0, c, buf.at[c + 1], scale, shift)
            pieces = [buf[c + 1, dr:dr + segrows].reshape(px, LANES) for dr in range(3)]
            prod = lax.dot_general(head_w[...], jnp.concatenate(pieces, axis=1), (((1,), (1,)), ((), ())), preferred_element_type=F32)
            for kc in range(3):
                part[c + 1, kc] = prod[kc * 8:kc * 8 + 8]
            return 0

        lax.fori_loop(0, cols, column_product, 0)
        q_send[i] = part[edge + 1, 2 * sx][0:4]
        edge_copy(i).start()
        slot = lax.rem(i, 4)
        for c in range(cols):
            y = part[c, 0] + part[c + 1, 1] + part[c + 2, 2]
            for ch in range(3):
                image[slot, ch * cols + c:ch * cols + c + 1, :] = y[ch:ch + 1]

    def head_finish(i):
        edge_copy(i).wait()
        slot = lax.rem(i, 4)
        for ch in range(3):
            at = pl.ds(ch * cols + edge, 1)
            image[slot, at, :] = image[slot, at, :] + q_recv[i][ch:ch + 1]
        y = image[slot]
        high = y.astype(BF16).astype(F32)
        rest = y - high
        mid = rest.astype(BF16).astype(F32)
        split = jnp.concatenate([high, mid, rest - mid], axis=0).astype(BF16)
        moved = jnp.dot(split, order[...], preferred_element_type=F32)
        n = 3 * cols
        moved = moved[0:n] + (moved[n:2 * n] + moved[2 * n:3 * n])
        shift = bo_ref[...].astype(F32)
        for ch in range(3):
            out_ref[i, ch] = moved[ch * cols:(ch + 1) * cols] + shift[0:1, ch:ch + 1]

    def nothing(i):
        pass

    def head(i):
        @pl.when(i >= 2)
        def _():
            head_products(i - 2)

        @pl.when(i >= 4)
        def _():
            head_finish(i - 4)

    run_layer(0, True, first_pair, lambda: w_one[...].reshape(24 * LANES, 2 * LANES), bias_f[0:1], False, False, False, nothing)
    run_layer(1, False, rest_pair(0), lambda: w_two[...].reshape(16 * LANES, 2 * LANES), bias_f[1:2] + bias_f[6:7], True, False, False, nothing)
    for at in range(4):
        weights = functools.partial(lambda n: w_mid[n].reshape(12 * LANES, 2 * LANES), at)
        run_layer(at % 2, False, rest_pair(at + 1), weights, bias_f[at + 2:at + 3], False, at % 2 == 1, at == 3, head if at == 3 else nothing)

    def tail(i, _):
        @pl.when(i < samples + 2)
        def _():
            head_products(i - 2)

        head_finish(i - 4)
        return 0

    lax.fori_loop(samples, samples + 4, tail, 0)


def solution(mesh):
    n_sy = mesh.shape["sy"]
    n_sx = mesh.shape["sx"]
    devices = n_sx * n_sy
    tile_spec = P("dp", "sy", "sx", None)
    replicated = P()

    def local_decode(act_in, norm_first, w_first, w_short, norm_rest, w_rest, bias_rest, w_out, bias_out):
        samples, rows, cols, chans = act_in.shape
        segrows = rows // SEGS
        act_five = act_in.reshape(samples, SEGS, segrows, cols, chans)
        w_head = jnp.transpose(w_out, (0, 1, 3, 2))
        vmem = pl.BlockSpec(memory_space=pltpu.VMEM)
        hbm = pl.BlockSpec(memory_space=pl.ANY)
        dma = pltpu.SemaphoreType.DMA
        scratch = [
            pltpu.VMEM((samples, 2, cols, segrows, SEGS, LANES), BF16),
            pltpu.VMEM((samples, cols, segrows, SEGS, LANES), BF16),
            pltpu.VMEM((2, cols + 2, segrows + 2, SEGS, LANES), BF16),
            pltpu.VMEM((2, cols + 2, segrows + 2, SEGS, LANES), BF16),
            pltpu.VMEM((3, 4, 2 * LANES, 2 * LANES), BF16),
            pltpu.VMEM((4, 4, LANES, 2 * LANES), BF16),
            pltpu.VMEM((4, 3, 4, LANES, 2 * LANES), BF16),
            pltpu.VMEM((samples, 2, segrows, SEGS, LANES), BF16),
            pltpu.VMEM((samples, segrows, SEGS, LANES), BF16),
            pltpu.VMEM((2, SEGS, segrows, cols, chans), BF16),
            pltpu.VMEM((2, SEGS * cols, LANES), F32),
            pltpu.VMEM((7, LANES), F32),
            pltpu.VMEM((samples, 2, 2, cols, LANES), F32),
            pltpu.VMEM((2, samples, 2, 2, cols, LANES), F32),
            pltpu.VMEM((samples, 2, 2, 1, LANES), F32),
            pltpu.VMEM((2, samples, 2, 2, 1, LANES), F32),
            pltpu.VMEM((2, samples, devices, 2, 2, LANES), F32),
            pltpu.VMEM((2, 2 * (devices - 1) + 2 * cols + 2, LANES), F32),
            pltpu.VMEM((32, 3 * LANES), F32),
            pltpu.VMEM((32, 3 * LANES), BF16),
            pltpu.VMEM((segrows * SEGS, segrows * SEGS), BF16),
            pltpu.VMEM((cols + 2, 3, 8, segrows * SEGS), F32),
            pltpu.VMEM((4, 3 * cols, segrows * SEGS), F32),
            pltpu.VMEM((samples, 4, segrows * SEGS), F32),
            pltpu.VMEM((samples, 4, segrows * SEGS), F32),
            dma((2,)),
            dma((40,)),
            dma((2, samples)),
            dma((2, samples)),
            dma((2, samples)),
            dma((2, samples)),
            dma((samples,)),
            dma((samples,)),
        ]
        cfg = (samples, segrows, cols, n_sx, n_sy)
        image = pl.pallas_call(
            functools.partial(decode_kernel, cfg),
            out_shape=jax.ShapeDtypeStruct((samples, 3, cols, rows), F32),
            in_specs=[hbm, vmem, hbm, hbm, vmem, hbm, vmem, vmem, vmem],
            out_specs=vmem,
            scratch_shapes=scratch,
            compiler_params=pltpu.CompilerParams(collective_id=0, has_side_effects=True, vmem_limit_bytes=67043328),
        )(act_five, norm_first, w_first, w_short, norm_rest, w_rest, bias_rest, w_head, bias_out.reshape(1, 3))
        return jnp.transpose(image, (0, 3, 2, 1))

    return jax.shard_map(local_decode, mesh=mesh, in_specs=(tile_spec, replicated, replicated, replicated, replicated, replicated, replicated, replicated, replicated), out_specs=tile_spec, check_vma=False)
```

```python
import functools

import jax
import jax.numpy as jnp
from jax import lax
from jax.experimental import pallas as pl
from jax.experimental.pallas import tpu as pltpu
from jax.sharding import PartitionSpec as P

GROUPS = 32
GN_EPS = 1e-6
DEFER = 7
HEAD_LAG = 4
EDGE_LAG = 6
LANES = 128
SEGS = 16
MESH = pl.DeviceIdType.MESH
F32 = jnp.float32
BF16 = jnp.bfloat16


def decode_kernel(cfg, a_hbm, nf_ref, wf_hbm, ws_hbm, nr_ref, wr_hbm, br_ref, wo_ref, bo_ref, out_ref,
                  wide, thin, act_a, act_b, w_one, w_two, w_mid, halo_even, halo_odd, land, shuffle, bias_f,
                  row_send, row_recv, cor_send, cor_recv, stat, tally, head_f, head_w, order, part, image, q_send, q_recv,
                  land_sem, w_sem, col_ss, col_rs, small_ss, small_rs, q_ss, q_rs):
    samples, segrows, cols, n_sx, n_sy = cfg
    devices = n_sx * n_sy
    px = segrows * SEGS
    sx = lax.axis_index("sx")
    sy = lax.axis_index("sy")
    me = sx * n_sy + sy
    edge = (cols - 1) * (1 - sx)
    pixels = segrows * SEGS * cols * devices
    acts = (act_a, act_b)

    barrier = pltpu.get_barrier_semaphore()
    peers = []
    for k in range(1, devices):
        peers.append({"sx": lax.rem(sx + k // n_sy, n_sx), "sy": lax.rem(sy + k % n_sy, n_sy)})
    for peer in peers:
        pl.semaphore_signal(barrier, inc=1, device_id=peer, device_id_type=MESH)

    def land_copy(i, slot):
        return pltpu.make_async_copy(a_hbm.at[i], land.at[slot], land_sem.at[slot])

    land_copy(0, 0).start()

    weight_copies = []
    for e in range(2):
        lanes = pl.ds(e * LANES, LANES)
        for dr in range(3):
            weight_copies.append((wf_hbm.at[dr], w_one.at[dr, pl.ds(e, 3), :, lanes]))
            weight_copies.append((wr_hbm.at[0, dr], w_two.at[dr, pl.ds(e, 3), :, lanes]))
            for layer in range(4):
                weight_copies.append((wr_hbm.at[layer + 1, dr], w_mid.at[layer, dr, pl.ds(e, 3), :, lanes]))
        for half in range(2):
            weight_copies.append((ws_hbm.at[pl.ds(half * LANES, LANES)], w_two.at[3, 2 * e + half, :, lanes]))
    weight_copies = [pltpu.make_async_copy(src, dst, w_sem.at[n]) for n, (src, dst) in enumerate(weight_copies)]

    pl.semaphore_wait(barrier, devices - 1)

    def column_copy(par, first, i):
        if first:
            src, dst = wide.at[i, :, edge], halo_even.at[i]
        elif par == 0:
            src, dst = wide.at[i, 0, edge], halo_even.at[i, 0]
        else:
            src, dst = thin.at[i, edge], halo_odd.at[i]
        return pltpu.make_async_remote_copy(
            src_ref=src, dst_ref=dst, send_sem=col_ss.at[par, i], recv_sem=col_rs.at[par, i],
            device_id={"sx": 1 - sx, "sy": sy}, device_id_type=MESH)

    def small_copies(par, first, i):
        pick = (lambda ref: ref) if first else (lambda ref: ref.at[0])
        mine = pick(stat.at[par, i, me])
        found = [(mine, mine, peer) for peer in peers]
        for t in range(2):
            other = lax.rem(sy + (n_sy - 1 if t == 0 else 1), n_sy)
            found.append((pick(row_send.at[i, t]), pick(row_recv.at[par, i, 1 - t]), {"sx": sx, "sy": other}))
            found.append((pick(cor_send.at[i, t]), pick(cor_recv.at[par, i, 1 - t]), {"sx": 1 - sx, "sy": other}))
        return [
            pltpu.make_async_remote_copy(src_ref=src, dst_ref=dst, send_sem=small_ss.at[par, i], recv_sem=small_rs.at[par, i], device_id=peer, device_id_type=MESH)
            for src, dst, peer in found
        ]

    def await_copies(par, first, i, with_column):
        size = tally if first else tally.at[0]
        pltpu.make_async_copy(size, size, small_ss.at[par, i]).wait()
        pltpu.make_async_copy(size, size, small_rs.at[par, i]).wait()
        if with_column:
            column_copy(par, first, i).wait()

    def send(par, first, i, sums, with_column):
        buf = wide if par == 0 else thin
        for half in range(2 if first else 1):
            stat[par, i, me, half] = jnp.concatenate([jnp.sum(part_sum, axis=0, keepdims=True) for part_sum in sums[half]], axis=0)
            for t in range(2):
                for c in range(cols):
                    at = (i, half, c) if par == 0 else (i, c)
                    tile = buf[at + (t * (segrows - 1),)].astype(F32)
                    row_send[i, t, half, pl.ds(c, 1), :] = tile[t * (SEGS - 1):t * (SEGS - 1) + 1]
                cor_send[i, t, half] = row_send[i, t, half, pl.ds(edge, 1), :]
        for copy in small_copies(par, first, i):
            copy.start()
        if with_column:
            column_copy(par, first, i).start()

    def prepare(i, _):
        slot = lax.rem(i, 2)
        land_copy(i, slot).wait()

        @pl.when(i + 1 < samples)
        def _():
            land_copy(i + 1, 1 - slot).start()

        def relayout(r, sums):
            new = []
            for half in range(2):
                block = land[slot, :, r, :, pl.ds(half * LANES, LANES)].astype(F32)
                s_one, s_two = sums[half]
                new.append((s_one + jnp.sum(block, axis=0), s_two + jnp.sum(block * block, axis=0)))
                shuffle[half] = block.reshape(SEGS * cols, LANES)
                for c in range(cols):
                    wide[i, half, c, r] = shuffle[half, pl.ds(c, SEGS, stride=cols), :].astype(BF16)
            return tuple(new)

        zero = jnp.zeros((8, LANES), F32)
        sums = lax.fori_loop(0, segrows, relayout, ((zero, zero), (zero, zero)))
        send(0, True, i, sums, True)
        return 0

    prepare(0, 0)
    for copy in weight_copies:
        copy.start()
    zero_one = jnp.zeros((2 * LANES, LANES), BF16)
    zero_block = jnp.zeros((LANES, LANES), BF16)
    for e in range(2):
        lanes = slice(e * LANES, (e + 1) * LANES)
        for dr in range(3):
            w_one[dr, 3 - 3 * e, :, lanes] = zero_one
            w_two[dr, 3 - 3 * e, :, lanes] = zero_block
            for layer in range(4):
                w_mid[layer, dr, 3 - 3 * e, :, lanes] = zero_block
        for half in range(2):
            w_two[3, 2 * (1 - e) + half, :, lanes] = zero_block
    bias_f[...] = br_ref[...].astype(F32)
    zero_col = (cols + 1) * sx
    for half in range(2):
        for buf in acts:
            buf[half, zero_col] = jnp.zeros((segrows + 2, SEGS, LANES), BF16)
    head_f[...] = jnp.zeros(head_f.shape, F32)
    for dr in range(3):
        for kc in range(3):
            for e in range(2):
                at = 72 * e + 24 * dr + 8 * kc
                head_f[at:at + 3, e * LANES:(e + 1) * LANES] = wo_ref[dr, kc].astype(F32)
    head_w[...] = head_f[...].astype(BF16)
    came = lax.broadcasted_iota(jnp.int32, (px, px), 0)
    goes = lax.broadcasted_iota(jnp.int32, (px, px), 1)
    order[...] = jnp.where(goes == lax.rem(came, SEGS) * segrows + lax.div(came, SEGS), 1.0, 0.0).astype(BF16)
    part[0, 0] = jnp.zeros((8, px), F32)
    part[cols + 1, 2] = jnp.zeros((8, px), F32)

    lax.fori_loop(1, samples, prepare, 0)
    for copy in weight_copies:
        copy.wait()

    lane = lax.broadcasted_iota(jnp.int32, (2, LANES), 1)
    seg_at = lax.broadcasted_iota(jnp.int32, (SEGS, LANES), 0)

    def group_total(x, size):
        step = 1
        while step < size:
            x = x + jnp.where((lane & step) != 0, pltpu.roll(x, step, 1), pltpu.roll(x, LANES - step, 1))
            step *= 2
        return x

    def silu_half(x, scale, shift):
        v = x * scale + shift
        return v + v * jnp.tanh(v)

    def norms(par, first, i, pair_of):
        per_group = (2 if first else 1) * LANES // GROUPS
        count = pixels * per_group
        found = []
        for half in range(2 if first else 1):
            total = stat[par, i, 0, half]
            for dev in range(1, devices):
                total = total + stat[par, i, dev, half]
            total = group_total(total, per_group) * (1.0 / count)
            mean, square = total[0:1], total[1:2]
            gamma, beta = pair_of(half)
            scale = gamma * lax.rsqrt(square - mean * mean + GN_EPS)
            shift = beta - mean * scale
            found.append((0.5 * scale, 0.5 * shift))
        return found

    def column(src, above, below, dst, scale, shift):
        z = silu_half(src.astype(F32), scale, shift)
        dst[1:segrows + 1] = z.astype(BF16)
        above = jnp.where(sy > 0, silu_half(above, scale, shift), 0.0)
        below = jnp.where(sy < n_sy - 1, silu_half(below, scale, shift), 0.0)
        dst[0] = jnp.where(seg_at == 0, above, pltpu.roll(z[segrows - 1], 1, 0)).astype(BF16)
        dst[segrows + 1] = jnp.where(seg_at == SEGS - 1, below, pltpu.roll(z[0], SEGS - 1, 0)).astype(BF16)

    def own_column(par, i, half, c, dst, scale, shift):
        src = wide[i, half, c] if par == 0 else thin[i, c]
        column(src, row_recv[par, i, 0, half, pl.ds(c, 1), :], row_recv[par, i, 1, half, pl.ds(c, 1), :], dst, scale, shift)

    def halo_column(par, first, i, buf, factors):
        for half, (scale, shift) in enumerate(factors):
            src = halo_even[i, half] if par == 0 else halo_odd[i]
            column(src, cor_recv[par, i, 0, half], cor_recv[par, i, 1, half], buf.at[half, (cols + 1) * (1 - sx)], scale, shift)

    def run_layer(par, first, pair_of, weights, bias, skip, residual, last, after):
        halves = 2 if first else 1

        await_copies(par, first, 0, True)
        start = norms(par, first, 0, pair_of)
        halo_column(par, first, 0, act_a, start)

        def own(c, _):
            for half, (scale, shift) in enumerate(start):
                own_column(par, 0, half, c, act_a.at[half, c + 1], scale, shift)
            return 0

        lax.fori_loop(0, cols, own, 0)

        def step(i, s):
            now, later = acts[s], acts[1 - s]
            if s == 0:
                ahead = i + 1
                await_copies(par, first, ahead, True)
            else:
                ahead = jnp.minimum(i + 1, samples - 1)

                @pl.when(i + 1 < samples)
                def _():
                    await_copies(par, first, ahead, True)

            factors = norms(par, first, ahead, pair_of)
            halo_column(par, first, ahead, later, factors)

            def quad(t, sums):
                rows_of = []
                for q in range(2):
                    p = 2 * t + q
                    pieces = []
                    for dr in range(3):
                        for j in range(4):
                            for half in range(halves):
                                pieces.append(now[half, 2 * p + j, dr:dr + segrows].reshape(px, LANES))
                    if skip:
                        for e in range(2):
                            for half in range(2):
                                pieces.append(wide[i, half, 2 * p + e].reshape(px, LANES))
                    rows_of.append(jnp.concatenate(pieces, axis=1))
                res = jnp.dot(jnp.concatenate(rows_of, axis=0), weights(), preferred_element_type=F32)
                for half, (scale, shift) in enumerate(factors):
                    for e in range(4):
                        own_column(par, ahead, half, 4 * t + e, later.at[half, 4 * t + e + 1], scale, shift)
                s_one, s_two = sums
                for q in range(2):
                    for e in range(2):
                        c = 4 * t + 2 * q + e
                        y = res[q * px:(q + 1) * px, e * LANES:(e + 1) * LANES] + bias
                        if residual:
                            y = y + wide[i, 0, c].reshape(px, LANES).astype(F32)
                        rounded = y.astype(BF16)
                        if par == 0:
                            thin[i, c] = rounded.reshape(segrows, SEGS, LANES)
                        else:
                            wide[i, 0, c] = rounded.reshape(segrows, SEGS, LANES)
                        back = rounded.astype(F32).reshape(px // 8, 8, LANES)
                        s_one = s_one + jnp.sum(back, axis=0)
                        s_two = s_two + jnp.sum(back * back, axis=0)
                return s_one, s_two

            zero = jnp.zeros((8, LANES), F32)
            sums = lax.fori_loop(0, cols // 4, quad, (zero, zero))
            send(1 - par, False, i, [sums], False)
            if not last:
                @pl.when(i >= DEFER)
                def _():
                    column_copy(1 - par, False, i - DEFER).start()

            if not first:
                @pl.when(i < DEFER)
                def _():
                    column_copy(par, False, i + samples - DEFER).start()

            after(i)

        def two(t, _):
            step(2 * t, 0)
            step(2 * t + 1, 1)
            return 0

        lax.fori_loop(0, samples // 2, two, 0)

    def rest_pair(at):
        def pair_of(half):
            pair = nr_ref[at].astype(F32)
            return pair[0:1], pair[1:2]
        return pair_of

    def first_pair(half):
        pair = nf_ref[:, half * LANES:(half + 1) * LANES].astype(F32)
        return pair[0:1], pair[1:2]

    def edge_copy(i):
        return pltpu.make_async_remote_copy(
            src_ref=q_send.at[i], dst_ref=q_recv.at[i], send_sem=q_ss.at[i], recv_sem=q_rs.at[i],
            device_id={"sx": 1 - sx, "sy": sy}, device_id_type=MESH)

    def head_products(i):
        await_copies(0, False, i, False)
        (scale, shift), = norms(0, False, i, rest_pair(5))
        buf = act_b.at[1]

        for c in range(0, cols, 2):
            for e in range(2):
                own_column(0, i, 0, c + e, buf.at[c + e + 1], scale, shift)
            both = jnp.concatenate([buf[c + e + 1].reshape(px + 2 * SEGS, LANES) for e in range(2)], axis=1)
            prod = lax.dot_general(head_w[...], both, (((1,), (1,)), ((), ())), preferred_element_type=F32)
            for e in range(2):
                for kc in range(3):
                    at = [72 * e + 24 * dr + 8 * kc for dr in range(3)]
                    part[c + e + 1, kc] = sum(prod[at[dr]:at[dr] + 8, dr * SEGS:dr * SEGS + px] for dr in range(3))
        q_send[i] = part[edge + 1, 2 * sx][0:4]
        edge_copy(i).start()
        slot = lax.rem(i, 4)
        for c in range(cols):
            y = part[c, 0] + part[c + 1, 1] + part[c + 2, 2]
            for ch in range(3):
                image[slot, ch * cols + c:ch * cols + c + 1, :] = y[ch:ch + 1]

    def head_finish(i):
        edge_copy(i).wait()
        slot = lax.rem(i, 4)
        for ch in range(3):
            at = pl.ds(ch * cols + edge, 1)
            image[slot, at, :] = image[slot, at, :] + q_recv[i][ch:ch + 1]
        y = image[slot]
        high = y.astype(BF16).astype(F32)
        rest = y - high
        mid = rest.astype(BF16).astype(F32)
        split = jnp.concatenate([high, mid, rest - mid], axis=0).astype(BF16)
        moved = jnp.dot(split, order[...], preferred_element_type=F32)
        n = 3 * cols
        moved = moved[0:n] + (moved[n:2 * n] + moved[2 * n:3 * n])
        shift = bo_ref[...].astype(F32)
        for ch in range(3):
            out_ref[i, ch] = moved[ch * cols:(ch + 1) * cols] + shift[0:1, ch:ch + 1]

    def nothing(i):
        pass

    def head(i):
        @pl.when(i >= HEAD_LAG)
        def _():
            head_products(i - HEAD_LAG)

        @pl.when(i >= EDGE_LAG)
        def _():
            head_finish(i - EDGE_LAG)

    run_layer(0, True, first_pair, lambda: w_one[...].reshape(24 * LANES, 2 * LANES), bias_f[0:1], False, False, False, nothing)
    run_layer(1, False, rest_pair(0), lambda: w_two[...].reshape(16 * LANES, 2 * LANES), bias_f[1:2] + bias_f[6:7], True, False, False, nothing)
    for at in range(4):
        weights = functools.partial(lambda n: w_mid[n].reshape(12 * LANES, 2 * LANES), at)
        run_layer(at % 2, False, rest_pair(at + 1), weights, bias_f[at + 2:at + 3], False, at % 2 == 1, at == 3, head if at == 3 else nothing)

    def tail(i, _):
        @pl.when(i < samples + HEAD_LAG)
        def _():
            head_products(i - HEAD_LAG)

        head_finish(i - EDGE_LAG)
        return 0

    lax.fori_loop(samples, samples + EDGE_LAG, tail, 0)


def solution(mesh):
    n_sy = mesh.shape["sy"]
    n_sx = mesh.shape["sx"]
    devices = n_sx * n_sy
    tile_spec = P("dp", "sy", "sx", None)
    replicated = P()

    def local_decode(act_in, norm_first, w_first, w_short, norm_rest, w_rest, bias_rest, w_out, bias_out):
        samples, rows, cols, chans = act_in.shape
        segrows = rows // SEGS
        act_five = act_in.reshape(samples, SEGS, segrows, cols, chans)
        w_head = jnp.transpose(w_out, (0, 1, 3, 2))
        vmem = pl.BlockSpec(memory_space=pltpu.VMEM)
        hbm = pl.BlockSpec(memory_space=pl.ANY)
        dma = pltpu.SemaphoreType.DMA
        scratch = [
            pltpu.VMEM((samples, 2, cols, segrows, SEGS, LANES), BF16),
            pltpu.VMEM((samples, cols, segrows, SEGS, LANES), BF16),
            pltpu.VMEM((2, cols + 2, segrows + 2, SEGS, LANES), BF16),
            pltpu.VMEM((2, cols + 2, segrows + 2, SEGS, LANES), BF16),
            pltpu.VMEM((3, 4, 2 * LANES, 2 * LANES), BF16),
            pltpu.VMEM((4, 4, LANES, 2 * LANES), BF16),
            pltpu.VMEM((4, 3, 4, LANES, 2 * LANES), BF16),
            pltpu.VMEM((samples, 2, segrows, SEGS, LANES), BF16),
            pltpu.VMEM((samples, segrows, SEGS, LANES), BF16),
            pltpu.VMEM((2, SEGS, segrows, cols, chans), BF16),
            pltpu.VMEM((2, SEGS * cols, LANES), F32),
            pltpu.VMEM((7, LANES), F32),
            pltpu.VMEM((samples, 2, 2, cols, LANES), F32),
            pltpu.VMEM((2, samples, 2, 2, cols, LANES), F32),
            pltpu.VMEM((samples, 2, 2, 1, LANES), F32),
            pltpu.VMEM((2, samples, 2, 2, 1, LANES), F32),
            pltpu.VMEM((2, samples, devices, 2, 2, LANES), F32),
            pltpu.VMEM((2, 2 * (devices - 1) + 2 * cols + 2, LANES), F32),
            pltpu.VMEM((144, 2 * LANES), F32),
            pltpu.VMEM((144, 2 * LANES), BF16),
            pltpu.VMEM((segrows * SEGS, segrows * SEGS), BF16),
            pltpu.VMEM((cols + 2, 3, 8, segrows * SEGS), F32),
            pltpu.VMEM((4, 3 * cols, segrows * SEGS), F32),
            pltpu.VMEM((samples, 4, segrows * SEGS), F32),
            pltpu.VMEM((samples, 4, segrows * SEGS), F32),
            dma((2,)),
            dma((40,)),
            dma((2, samples)),
            dma((2, samples)),
            dma((2, samples)),
            dma((2, samples)),
            dma((samples,)),
            dma((samples,)),
        ]
        cfg = (samples, segrows, cols, n_sx, n_sy)
        image = pl.pallas_call(
            functools.partial(decode_kernel, cfg),
            out_shape=jax.ShapeDtypeStruct((samples, 3, cols, rows), F32),
            in_specs=[hbm, vmem, hbm, hbm, vmem, hbm, vmem, vmem, vmem],
            out_specs=vmem,
            scratch_shapes=scratch,
            compiler_params=pltpu.CompilerParams(collective_id=0, has_side_effects=True, vmem_limit_bytes=67043328),
        )(act_five, norm_first, w_first, w_short, norm_rest, w_rest, bias_rest, w_head, bias_out.reshape(1, 3))
        return jnp.transpose(image, (0, 3, 2, 1))

    return jax.shard_map(local_decode, mesh=mesh, in_specs=(tile_spec, replicated, replicated, replicated, replicated, replicated, replicated, replicated, replicated), out_specs=tile_spec, check_vma=False)
```

```python
import functools

import jax
import jax.numpy as jnp
from jax import lax
from jax.experimental import pallas as pl
from jax.experimental.pallas import tpu as pltpu
from jax.sharding import PartitionSpec as P

GROUPS = 32
GN_EPS = 1e-6
DEFER = 8
HEAD_LAG = 3
EDGE_LAG = 5
LANES = 128
SEGS = 16
MESH = pl.DeviceIdType.MESH
F32 = jnp.float32
BF16 = jnp.bfloat16


def decode_kernel(cfg, a_hbm, nf_ref, wf_hbm, ws_hbm, nr_ref, wr_hbm, br_ref, wo_ref, bo_ref, out_ref,
                  wide, thin, act_a, act_b, w_one, w_two, w_mid, halo_even, halo_odd, land, shuffle, bias_f,
                  row_send, row_recv, cor_send, cor_recv, stat, tally, head_f, head_w, order, image, q_send, q_recv,
                  land_sem, w_sem, col_ss, col_rs, small_ss, small_rs, q_ss, q_rs):
    samples, segrows, cols, n_sx, n_sy = cfg
    devices = n_sx * n_sy
    px = segrows * SEGS
    sx = lax.axis_index("sx")
    sy = lax.axis_index("sy")
    me = sx * n_sy + sy
    edge = (cols - 1) * (1 - sx)
    pixels = segrows * SEGS * cols * devices
    acts = (act_a, act_b)

    barrier = pltpu.get_barrier_semaphore()
    peers = []
    for k in range(1, devices):
        peers.append({"sx": lax.rem(sx + k // n_sy, n_sx), "sy": lax.rem(sy + k % n_sy, n_sy)})
    for peer in peers:
        pl.semaphore_signal(barrier, inc=1, device_id=peer, device_id_type=MESH)

    def land_copy(i, slot):
        return pltpu.make_async_copy(a_hbm.at[i], land.at[slot], land_sem.at[slot])

    def land_start(i, slot):
        for at in range(0, SEGS, 2):
            rows = pl.ds(at, 2)
            pltpu.make_async_copy(a_hbm.at[i, rows], land.at[slot, rows], land_sem.at[slot]).start()

    land_start(0, 0)

    weight_copies = []
    for e in range(2):
        lanes = pl.ds(e * LANES, LANES)
        for dr in range(3):
            weight_copies.append((wf_hbm.at[dr], w_one.at[dr, pl.ds(e, 3), :, lanes]))
            weight_copies.append((wr_hbm.at[0, dr], w_two.at[dr, pl.ds(e, 3), :, lanes]))
            for layer in range(4):
                weight_copies.append((wr_hbm.at[layer + 1, dr], w_mid.at[layer, dr, pl.ds(e, 3), :, lanes]))
        for half in range(2):
            weight_copies.append((ws_hbm.at[pl.ds(half * LANES, LANES)], w_two.at[3, 2 * e + half, :, lanes]))
    weight_copies = [pltpu.make_async_copy(src, dst, w_sem.at[n]) for n, (src, dst) in enumerate(weight_copies)]

    def column_copy(par, first, i):
        if first:
            src, dst = wide.at[i, :, edge], halo_even.at[i]
        elif par == 0:
            src, dst = wide.at[i, 0, edge], halo_even.at[i, 0]
        else:
            src, dst = thin.at[i, edge], halo_odd.at[i]
        return pltpu.make_async_remote_copy(
            src_ref=src, dst_ref=dst, send_sem=col_ss.at[par, i], recv_sem=col_rs.at[par, i],
            device_id={"sx": 1 - sx, "sy": sy}, device_id_type=MESH)

    def small_copies(par, first, i):
        pick = (lambda ref: ref) if first else (lambda ref: ref.at[0])
        mine = pick(stat.at[par, i, me])
        found = [(mine, mine, peer) for peer in peers]
        for t in range(2):
            other = lax.rem(sy + (n_sy - 1 if t == 0 else 1), n_sy)
            found.append((pick(row_send.at[i, t]), pick(row_recv.at[par, i, 1 - t]), {"sx": sx, "sy": other}))
            found.append((pick(cor_send.at[i, t]), pick(cor_recv.at[par, i, 1 - t]), {"sx": 1 - sx, "sy": other}))
        return [
            pltpu.make_async_remote_copy(src_ref=src, dst_ref=dst, send_sem=small_ss.at[par, i], recv_sem=small_rs.at[par, i], device_id=peer, device_id_type=MESH)
            for src, dst, peer in found
        ]

    def await_copies(par, first, i, with_column):
        size = tally if first else tally.at[0]
        pltpu.make_async_copy(size, size, small_ss.at[par, i]).wait()
        pltpu.make_async_copy(size, size, small_rs.at[par, i]).wait()
        if with_column:
            column_copy(par, first, i).wait()

    def send(par, first, i, sums, with_column):
        buf = wide if par == 0 else thin
        for half in range(2 if first else 1):
            stat[par, i, me, half] = jnp.concatenate([jnp.sum(part_sum, axis=0, keepdims=True) for part_sum in sums[half]], axis=0)
            for t in range(2):
                for c in range(cols):
                    at = (i, half, c) if par == 0 else (i, c)
                    tile = buf[at + (t * (segrows - 1),)].astype(F32)
                    row_send[i, t, half, pl.ds(c, 1), :] = tile[t * (SEGS - 1):t * (SEGS - 1) + 1]
                cor_send[i, t, half] = row_send[i, t, half, pl.ds(edge, 1), :]
        for copy in small_copies(par, first, i):
            copy.start()
        if with_column:
            column_copy(par, first, i).start()

    def prepare(i, begin):
        slot = lax.rem(i, 2)
        land_copy(i, slot).wait()

        @pl.when(i + 1 < samples)
        def _():
            land_start(i + 1, 1 - slot)

        def relayout(r, sums):
            new = []
            for half in range(2):
                block = land[slot, :, r, :, pl.ds(half * LANES, LANES)].astype(F32)
                s_one, s_two = sums[half]
                new.append((s_one + jnp.sum(block, axis=0), s_two + jnp.sum(block * block, axis=0)))
                shuffle[half] = block.reshape(SEGS * cols, LANES)
                for c in range(cols):
                    wide[i, half, c, r] = shuffle[half, pl.ds(c, SEGS, stride=cols), :].astype(BF16)
            return tuple(new)

        zero = jnp.zeros((8, LANES), F32)
        sums = lax.fori_loop(0, segrows, relayout, ((zero, zero), (zero, zero)))
        if begin is None:
            pl.semaphore_wait(barrier, devices - 1)
        send(0, True, i, sums, True)
        return 0

    prepare(0, None)
    for copy in weight_copies:
        copy.start()
    zero_one = jnp.zeros((2 * LANES, LANES), BF16)
    zero_block = jnp.zeros((LANES, LANES), BF16)
    for e in range(2):
        lanes = slice(e * LANES, (e + 1) * LANES)
        for dr in range(3):
            w_one[dr, 3 - 3 * e, :, lanes] = zero_one
            w_two[dr, 3 - 3 * e, :, lanes] = zero_block
            for layer in range(4):
                w_mid[layer, dr, 3 - 3 * e, :, lanes] = zero_block
        for half in range(2):
            w_two[3, 2 * (1 - e) + half, :, lanes] = zero_block
    bias_f[...] = br_ref[...].astype(F32)
    zero_col = (cols + 1) * sx
    for half in range(2):
        for buf in acts:
            buf[half, zero_col] = jnp.zeros((segrows + 2, SEGS, LANES), BF16)
    head_f[...] = jnp.zeros(head_f.shape, F32)
    for dr in range(3):
        for kc in range(3):
            for e in range(2):
                at = 72 * e + 24 * dr + 8 * kc
                head_f[at:at + 3, e * LANES:(e + 1) * LANES] = wo_ref[dr, kc].astype(F32)
    head_w[...] = head_f[...].astype(BF16)
    came = lax.broadcasted_iota(jnp.int32, (px, px), 0)
    goes = lax.broadcasted_iota(jnp.int32, (px, px), 1)
    order[...] = jnp.where(goes == lax.rem(came, SEGS) * segrows + lax.div(came, SEGS), 1.0, 0.0).astype(BF16)

    lax.fori_loop(1, samples, prepare, 0)
    for copy in weight_copies:
        copy.wait()

    lane = lax.broadcasted_iota(jnp.int32, (2, LANES), 1)
    seg_at = lax.broadcasted_iota(jnp.int32, (SEGS, LANES), 0)

    def group_total(x, size):
        step = 1
        while step < size:
            x = x + jnp.where((lane & step) != 0, pltpu.roll(x, step, 1), pltpu.roll(x, LANES - step, 1))
            step *= 2
        return x

    def silu_half(x, scale, shift):
        v = x * scale + shift
        return v + v * jnp.tanh(v)

    def norms(par, first, i, pair_of):
        per_group = (2 if first else 1) * LANES // GROUPS
        count = pixels * per_group
        found = []
        for half in range(2 if first else 1):
            total = stat[par, i, 0, half]
            for dev in range(1, devices):
                total = total + stat[par, i, dev, half]
            total = group_total(total, per_group) * (1.0 / count)
            mean, square = total[0:1], total[1:2]
            gamma, beta = pair_of(half)
            scale = gamma * lax.rsqrt(square - mean * mean + GN_EPS)
            shift = beta - mean * scale
            found.append((0.5 * scale, 0.5 * shift))
        return found

    def column(src, above, below, dst, scale, shift):
        z = silu_half(src.astype(F32), scale, shift)
        dst[1:segrows + 1] = z.astype(BF16)
        above = jnp.where(sy > 0, silu_half(above, scale, shift), 0.0)
        below = jnp.where(sy < n_sy - 1, silu_half(below, scale, shift), 0.0)
        dst[0] = jnp.where(seg_at == 0, above, pltpu.roll(z[segrows - 1], 1, 0)).astype(BF16)
        dst[segrows + 1] = jnp.where(seg_at == SEGS - 1, below, pltpu.roll(z[0], SEGS - 1, 0)).astype(BF16)

    def own_column(par, i, half, c, dst, scale, shift):
        src = wide[i, half, c] if par == 0 else thin[i, c]
        column(src, row_recv[par, i, 0, half, pl.ds(c, 1), :], row_recv[par, i, 1, half, pl.ds(c, 1), :], dst, scale, shift)

    def halo_column(par, first, i, buf, factors):
        for half, (scale, shift) in enumerate(factors):
            src = halo_even[i, half] if par == 0 else halo_odd[i]
            column(src, cor_recv[par, i, 0, half], cor_recv[par, i, 1, half], buf.at[half, (cols + 1) * (1 - sx)], scale, shift)

    def run_layer(par, first, pair_of, weights, bias, skip, residual, last, after):
        halves = 2 if first else 1

        await_copies(par, first, 0, True)
        start = norms(par, first, 0, pair_of)
        halo_column(par, first, 0, act_a, start)

        def own(c, _):
            for half, (scale, shift) in enumerate(start):
                own_column(par, 0, half, c, act_a.at[half, c + 1], scale, shift)
            return 0

        lax.fori_loop(0, cols, own, 0)

        def step(i, s):
            now, later = acts[s], acts[1 - s]
            if s == 0:
                ahead = i + 1
                await_copies(par, first, ahead, False)
            else:
                ahead = jnp.minimum(i + 1, samples - 1)

                @pl.when(i + 1 < samples)
                def _():
                    await_copies(par, first, ahead, False)

            factors = norms(par, first, ahead, pair_of)

            def quad(t, sums):
                rows_of = []
                for q in range(2):
                    p = 2 * t + q
                    pieces = []
                    for dr in range(3):
                        for j in range(4):
                            for half in range(halves):
                                pieces.append(now[half, 2 * p + j, dr:dr + segrows].reshape(px, LANES))
                    if skip:
                        for e in range(2):
                            for half in range(2):
                                pieces.append(wide[i, half, 2 * p + e].reshape(px, LANES))
                    rows_of.append(jnp.concatenate(pieces, axis=1))
                res = jnp.dot(jnp.concatenate(rows_of, axis=0), weights(), preferred_element_type=F32)
                for half, (scale, shift) in enumerate(factors):
                    for e in range(4):
                        own_column(par, ahead, half, 4 * t + e, later.at[half, 4 * t + e + 1], scale, shift)
                s_one, s_two = sums
                for q in range(2):
                    for e in range(2):
                        c = 4 * t + 2 * q + e
                        y = res[q * px:(q + 1) * px, e * LANES:(e + 1) * LANES] + bias
                        if residual:
                            y = y + wide[i, 0, c].reshape(px, LANES).astype(F32)
                        rounded = y.astype(BF16)
                        if par == 0:
                            thin[i, c] = rounded.reshape(segrows, SEGS, LANES)
                        else:
                            wide[i, 0, c] = rounded.reshape(segrows, SEGS, LANES)
                        back = rounded.astype(F32).reshape(px // 8, 8, LANES)
                        s_one = s_one + jnp.sum(back, axis=0)
                        s_two = s_two + jnp.sum(back * back, axis=0)
                return s_one, s_two

            zero = jnp.zeros((8, LANES), F32)
            sums = lax.fori_loop(0, cols // 4, quad, (zero, zero))
            send(1 - par, False, i, [sums], False)
            if not last:
                @pl.when(i >= DEFER)
                def _():
                    column_copy(1 - par, False, i - DEFER).start()

            if not first:
                @pl.when(i < DEFER)
                def _():
                    column_copy(par, False, i + samples - DEFER).start()

            after(i)
            if s == 0:
                column_copy(par, first, ahead).wait()
                halo_column(par, first, ahead, later, factors)
            else:
                @pl.when(i + 1 < samples)
                def _():
                    column_copy(par, first, ahead).wait()
                    halo_column(par, first, ahead, later, factors)

        def two(t, _):
            step(2 * t, 0)
            step(2 * t + 1, 1)
            return 0

        lax.fori_loop(0, samples // 2, two, 0)

    def rest_pair(at):
        def pair_of(half):
            pair = nr_ref[at].astype(F32)
            return pair[0:1], pair[1:2]
        return pair_of

    def first_pair(half):
        pair = nf_ref[:, half * LANES:(half + 1) * LANES].astype(F32)
        return pair[0:1], pair[1:2]

    def edge_copy(i):
        return pltpu.make_async_remote_copy(
            src_ref=q_send.at[i], dst_ref=q_recv.at[i], send_sem=q_ss.at[i], recv_sem=q_rs.at[i],
            device_id={"sx": 1 - sx, "sy": sy}, device_id_type=MESH)

    def head_products(i):
        await_copies(0, False, i, False)
        (scale, shift), = norms(0, False, i, rest_pair(5))
        buf = act_b.at[1]
        prods = []
        for c in range(0, cols, 2):
            for e in range(2):
                own_column(0, i, 0, c + e, buf.at[c + e + 1], scale, shift)
            both = jnp.concatenate([buf[c + e + 1].reshape(px + 2 * SEGS, LANES) for e in range(2)], axis=1)
            prods.append(lax.dot_general(head_w[...], both, (((1,), (1,)), ((), ())), preferred_element_type=F32))

        def tap(c, dr, kc):
            at = 72 * (c % 2) + 24 * dr + 8 * kc
            return prods[c // 2][at:at + 8]

        def shifted(taps):
            return sum(taps[dr][:, dr * SEGS:dr * SEGS + px] for dr in range(3))

        q_send[i] = shifted([jnp.where(sx == 0, tap(cols - 1, dr, 0), tap(0, dr, 2)) for dr in range(3)])[0:4]
        edge_copy(i).start()
        slot = lax.rem(i, 4)
        for c in range(cols):
            near = [kc for kc in range(3) if 0 <= c + kc - 1 < cols]
            y = shifted([sum(tap(c + kc - 1, dr, kc) for kc in near) for dr in range(3)])
            for ch in range(3):
                image[slot, ch * cols + c:ch * cols + c + 1, :] = y[ch:ch + 1]

    def head_finish(i):
        edge_copy(i).wait()
        slot = lax.rem(i, 4)
        for ch in range(3):
            at = pl.ds(ch * cols + edge, 1)
            image[slot, at, :] = image[slot, at, :] + q_recv[i][ch:ch + 1]
        y = image[slot]
        high = y.astype(BF16).astype(F32)
        rest = y - high
        mid = rest.astype(BF16).astype(F32)
        split = jnp.concatenate([high, mid, rest - mid], axis=0).astype(BF16)
        moved = jnp.dot(split, order[...], preferred_element_type=F32)
        n = 3 * cols
        moved = moved[0:n] + (moved[n:2 * n] + moved[2 * n:3 * n])
        shift = bo_ref[...].astype(F32)
        for ch in range(3):
            out_ref[i, ch] = moved[ch * cols:(ch + 1) * cols] + shift[0:1, ch:ch + 1]

    def nothing(i):
        pass

    def head(i):
        @pl.when(i >= HEAD_LAG)
        def _():
            head_products(i - HEAD_LAG)

        @pl.when(i >= EDGE_LAG)
        def _():
            head_finish(i - EDGE_LAG)

    run_layer(0, True, first_pair, lambda: w_one[...].reshape(24 * LANES, 2 * LANES), bias_f[0:1], False, False, False, nothing)
    run_layer(1, False, rest_pair(0), lambda: w_two[...].reshape(16 * LANES, 2 * LANES), bias_f[1:2] + bias_f[6:7], True, False, False, nothing)
    for at in range(4):
        weights = functools.partial(lambda n: w_mid[n].reshape(12 * LANES, 2 * LANES), at)
        run_layer(at % 2, False, rest_pair(at + 1), weights, bias_f[at + 2:at + 3], False, at % 2 == 1, at == 3, head if at == 3 else nothing)

    def tail(i, _):
        @pl.when(i < samples + HEAD_LAG)
        def _():
            head_products(i - HEAD_LAG)

        head_finish(i - EDGE_LAG)
        return 0

    lax.fori_loop(samples, samples + EDGE_LAG, tail, 0)


def solution(mesh):
    n_sy = mesh.shape["sy"]
    n_sx = mesh.shape["sx"]
    devices = n_sx * n_sy
    tile_spec = P("dp", "sy", "sx", None)
    replicated = P()

    def local_decode(act_in, norm_first, w_first, w_short, norm_rest, w_rest, bias_rest, w_out, bias_out):
        samples, rows, cols, chans = act_in.shape
        segrows = rows // SEGS
        act_five = act_in.reshape(samples, SEGS, segrows, cols, chans)
        w_head = jnp.transpose(w_out, (0, 1, 3, 2))
        vmem = pl.BlockSpec(memory_space=pltpu.VMEM)
        hbm = pl.BlockSpec(memory_space=pl.ANY)
        dma = pltpu.SemaphoreType.DMA
        scratch = [
            pltpu.VMEM((samples, 2, cols, segrows, SEGS, LANES), BF16),
            pltpu.VMEM((samples, cols, segrows, SEGS, LANES), BF16),
            pltpu.VMEM((2, cols + 2, segrows + 2, SEGS, LANES), BF16),
            pltpu.VMEM((2, cols + 2, segrows + 2, SEGS, LANES), BF16),
            pltpu.VMEM((3, 4, 2 * LANES, 2 * LANES), BF16),
            pltpu.VMEM((4, 4, LANES, 2 * LANES), BF16),
            pltpu.VMEM((4, 3, 4, LANES, 2 * LANES), BF16),
            pltpu.VMEM((samples, 2, segrows, SEGS, LANES), BF16),
            pltpu.VMEM((samples, segrows, SEGS, LANES), BF16),
            pltpu.VMEM((2, SEGS, segrows, cols, chans), BF16),
            pltpu.VMEM((2, SEGS * cols, LANES), F32),
            pltpu.VMEM((7, LANES), F32),
            pltpu.VMEM((samples, 2, 2, cols, LANES), F32),
            pltpu.VMEM((2, samples, 2, 2, cols, LANES), F32),
            pltpu.VMEM((samples, 2, 2, 1, LANES), F32),
            pltpu.VMEM((2, samples, 2, 2, 1, LANES), F32),
            pltpu.VMEM((2, samples, devices, 2, 2, LANES), F32),
            pltpu.VMEM((2, 2 * (devices - 1) + 2 * cols + 2, LANES), F32),
            pltpu.VMEM((144, 2 * LANES), F32),
            pltpu.VMEM((144, 2 * LANES), BF16),
            pltpu.VMEM((segrows * SEGS, segrows * SEGS), BF16),
            pltpu.VMEM((4, 3 * cols, segrows * SEGS), F32),
            pltpu.VMEM((samples, 4, segrows * SEGS), F32),
            pltpu.VMEM((samples, 4, segrows * SEGS), F32),
            dma((2,)),
            dma((40,)),
            dma((2, samples)),
            dma((2, samples)),
            dma((2, samples)),
            dma((2, samples)),
            dma((samples,)),
            dma((samples,)),
        ]
        cfg = (samples, segrows, cols, n_sx, n_sy)
        image = pl.pallas_call(
            functools.partial(decode_kernel, cfg),
            out_shape=jax.ShapeDtypeStruct((samples, 3, cols, rows), F32),
            in_specs=[hbm, vmem, hbm, hbm, vmem, hbm, vmem, vmem, vmem],
            out_specs=vmem,
            scratch_shapes=scratch,
            compiler_params=pltpu.CompilerParams(collective_id=0, has_side_effects=True, vmem_limit_bytes=67043328),
        )(act_five, norm_first, w_first, w_short, norm_rest, w_rest, bias_rest, w_head, bias_out.reshape(1, 3))
        return jnp.transpose(image, (0, 3, 2, 1))

    return jax.shard_map(local_decode, mesh=mesh, in_specs=(tile_spec, replicated, replicated, replicated, replicated, replicated, replicated, replicated, replicated), out_specs=tile_spec, check_vma=False)
```

```python
import functools

import jax
import jax.numpy as jnp
from jax import lax
from jax.experimental import pallas as pl
from jax.experimental.pallas import tpu as pltpu
from jax.sharding import PartitionSpec as P

GROUPS = 32
GN_EPS = 1e-6
DEFER = 9
HEAD_LAG = 3
EDGE_LAG = 5
LANES = 128
SEGS = 16
MESH = pl.DeviceIdType.MESH
F32 = jnp.float32
BF16 = jnp.bfloat16


def decode_kernel(cfg, a_hbm, nf_ref, wf_hbm, ws_hbm, nr_ref, wr_hbm, br_ref, wo_ref, bo_ref, out_ref,
                  wide, thin, act_a, act_b, w_one, w_two, w_mid, halo_even, halo_odd, land, shuffle, bias_f,
                  row_send, row_recv, cor_send, cor_recv, stat, tally, head_f, head_w, order, image, q_send, q_recv,
                  land_sem, w_sem, col_ss, col_rs, small_ss, small_rs, q_ss, q_rs):
    samples, segrows, cols, n_sx, n_sy = cfg
    devices = n_sx * n_sy
    px = segrows * SEGS
    sx = lax.axis_index("sx")
    sy = lax.axis_index("sy")
    me = sx * n_sy + sy
    edge = (cols - 1) * (1 - sx)
    pixels = segrows * SEGS * cols * devices
    acts = (act_a, act_b)

    barrier = pltpu.get_barrier_semaphore()
    peers = []
    for k in range(1, devices):
        peers.append({"sx": lax.rem(sx + k // n_sy, n_sx), "sy": lax.rem(sy + k % n_sy, n_sy)})
    for peer in peers:
        pl.semaphore_signal(barrier, inc=1, device_id=peer, device_id_type=MESH)

    def land_copy(i, slot):
        return pltpu.make_async_copy(a_hbm.at[i], land.at[slot], land_sem.at[slot])

    def land_start(i, slot):
        for at in range(0, SEGS, 2):
            rows = pl.ds(at, 2)
            pltpu.make_async_copy(a_hbm.at[i, rows], land.at[slot, rows], land_sem.at[slot]).start()

    land_start(0, 0)

    weight_copies = []
    for e in range(2):
        lanes = pl.ds(e * LANES, LANES)
        for dr in range(3):
            weight_copies.append((wf_hbm.at[dr], w_one.at[dr, pl.ds(e, 3), :, lanes]))
            weight_copies.append((wr_hbm.at[0, dr], w_two.at[dr, pl.ds(e, 3), :, lanes]))
            for layer in range(4):
                weight_copies.append((wr_hbm.at[layer + 1, dr], w_mid.at[layer, dr, pl.ds(e, 3), :, lanes]))
        for half in range(2):
            weight_copies.append((ws_hbm.at[pl.ds(half * LANES, LANES)], w_two.at[3, 2 * e + half, :, lanes]))
    weight_copies = [pltpu.make_async_copy(src, dst, w_sem.at[n]) for n, (src, dst) in enumerate(weight_copies)]

    def column_copy(par, first, i):
        if first:
            src, dst = wide.at[i, :, edge], halo_even.at[i]
        elif par == 0:
            src, dst = wide.at[i, 0, edge], halo_even.at[i, 0]
        else:
            src, dst = thin.at[i, edge], halo_odd.at[i]
        return pltpu.make_async_remote_copy(
            src_ref=src, dst_ref=dst, send_sem=col_ss.at[par, i], recv_sem=col_rs.at[par, i],
            device_id={"sx": 1 - sx, "sy": sy}, device_id_type=MESH)

    def small_copies(par, first, i):
        pick = (lambda ref: ref) if first else (lambda ref: ref.at[0])
        mine = pick(stat.at[par, i, me])
        found = [(mine, mine, peer) for peer in peers]
        for t in range(2):
            other = lax.rem(sy + (n_sy - 1 if t == 0 else 1), n_sy)
            found.append((pick(row_send.at[i, t]), pick(row_recv.at[par, i, 1 - t]), {"sx": sx, "sy": other}))
            found.append((pick(cor_send.at[i, t]), pick(cor_recv.at[par, i, 1 - t]), {"sx": 1 - sx, "sy": other}))
        return [
            pltpu.make_async_remote_copy(src_ref=src, dst_ref=dst, send_sem=small_ss.at[par, i], recv_sem=small_rs.at[par, i], device_id=peer, device_id_type=MESH)
            for src, dst, peer in found
        ]

    def await_copies(par, first, i, with_column):
        size = tally if first else tally.at[0]
        pltpu.make_async_copy(size, size, small_ss.at[par, i]).wait()
        pltpu.make_async_copy(size, size, small_rs.at[par, i]).wait()
        if with_column:
            column_copy(par, first, i).wait()

    def send(par, first, i, sums, with_column):
        buf = wide if par == 0 else thin
        for half in range(2 if first else 1):
            stat[par, i, me, half] = jnp.concatenate([jnp.sum(part_sum, axis=0, keepdims=True) for part_sum in sums[half]], axis=0)
            for t in range(2):
                for c in range(cols):
                    at = (i, half, c) if par == 0 else (i, c)
                    tile = buf[at + (t * (segrows - 1),)].astype(F32)
                    row_send[i, t, half, pl.ds(c, 1), :] = tile[t * (SEGS - 1):t * (SEGS - 1) + 1]
                cor_send[i, t, half] = row_send[i, t, half, pl.ds(edge, 1), :]
        for copy in small_copies(par, first, i):
            copy.start()
        if with_column:
            column_copy(par, first, i).start()

    def prepare(i, begin):
        slot = lax.rem(i, 2)
        land_copy(i, slot).wait()

        @pl.when(i + 1 < samples)
        def _():
            land_start(i + 1, 1 - slot)

        def relayout(r, sums):
            new = []
            for half in range(2):
                block = land[slot, :, r, :, pl.ds(half * LANES, LANES)].astype(F32)
                s_one, s_two = sums[half]
                new.append((s_one + jnp.sum(block, axis=0), s_two + jnp.sum(block * block, axis=0)))
                shuffle[half] = block.reshape(SEGS * cols, LANES)
                for c in range(cols):
                    wide[i, half, c, r] = shuffle[half, pl.ds(c, SEGS, stride=cols), :].astype(BF16)
            return tuple(new)

        zero = jnp.zeros((8, LANES), F32)
        sums = lax.fori_loop(0, segrows, relayout, ((zero, zero), (zero, zero)))
        if begin is None:
            pl.semaphore_wait(barrier, devices - 1)
        send(0, True, i, sums, True)
        return 0

    prepare(0, None)
    for copy in weight_copies:
        copy.start()
    zero_one = jnp.zeros((2 * LANES, LANES), BF16)
    zero_block = jnp.zeros((LANES, LANES), BF16)
    for e in range(2):
        lanes = slice(e * LANES, (e + 1) * LANES)
        for dr in range(3):
            w_one[dr, 3 - 3 * e, :, lanes] = zero_one
            w_two[dr, 3 - 3 * e, :, lanes] = zero_block
            for layer in range(4):
                w_mid[layer, dr, 3 - 3 * e, :, lanes] = zero_block
        for half in range(2):
            w_two[3, 2 * (1 - e) + half, :, lanes] = zero_block
    bias_f[...] = br_ref[...].astype(F32)
    zero_col = (cols + 1) * sx
    for half in range(2):
        for buf in acts:
            buf[half, zero_col] = jnp.zeros((segrows + 2, SEGS, LANES), BF16)
    head_f[...] = jnp.zeros(head_f.shape, F32)
    for dr in range(3):
        for kc in range(3):
            for e in range(2):
                at = 72 * e + 24 * dr + 8 * kc
                head_f[at:at + 3, e * LANES:(e + 1) * LANES] = wo_ref[dr, kc].astype(F32)
    head_w[...] = head_f[...].astype(BF16)
    came = lax.broadcasted_iota(jnp.int32, (px, px), 0)
    goes = lax.broadcasted_iota(jnp.int32, (px, px), 1)
    order[...] = jnp.where(goes == lax.rem(came, SEGS) * segrows + lax.div(came, SEGS), 1.0, 0.0).astype(BF16)

    lax.fori_loop(1, samples, prepare, 0)
    for copy in weight_copies:
        copy.wait()

    lane = lax.broadcasted_iota(jnp.int32, (2, LANES), 1)
    seg_at = lax.broadcasted_iota(jnp.int32, (SEGS, LANES), 0)

    def group_total(x, size):
        step = 1
        while step < size:
            x = x + jnp.where((lane & step) != 0, pltpu.roll(x, step, 1), pltpu.roll(x, LANES - step, 1))
            step *= 2
        return x

    def silu_half(x, scale, shift):
        v = x * scale + shift
        return v + v * jnp.tanh(v)

    def norms(par, first, i, pair_of):
        per_group = (2 if first else 1) * LANES // GROUPS
        count = pixels * per_group
        found = []
        for half in range(2 if first else 1):
            total = stat[par, i, 0, half]
            for dev in range(1, devices):
                total = total + stat[par, i, dev, half]
            total = group_total(total, per_group) * (1.0 / count)
            mean, square = total[0:1], total[1:2]
            gamma, beta = pair_of(half)
            scale = gamma * lax.rsqrt(square - mean * mean + GN_EPS)
            shift = beta - mean * scale
            found.append((0.5 * scale, 0.5 * shift))
        return found

    def column(src, above, below, dst, scale, shift):
        z = silu_half(src.astype(F32), scale, shift)
        dst[1:segrows + 1] = z.astype(BF16)
        above = jnp.where(sy > 0, silu_half(above, scale, shift), 0.0)
        below = jnp.where(sy < n_sy - 1, silu_half(below, scale, shift), 0.0)
        dst[0] = jnp.where(seg_at == 0, above, pltpu.roll(z[segrows - 1], 1, 0)).astype(BF16)
        dst[segrows + 1] = jnp.where(seg_at == SEGS - 1, below, pltpu.roll(z[0], SEGS - 1, 0)).astype(BF16)

    def own_column(par, i, half, c, dst, scale, shift):
        src = wide[i, half, c] if par == 0 else thin[i, c]
        column(src, row_recv[par, i, 0, half, pl.ds(c, 1), :], row_recv[par, i, 1, half, pl.ds(c, 1), :], dst, scale, shift)

    def halo_column(par, first, i, buf, factors):
        for half, (scale, shift) in enumerate(factors):
            src = halo_even[i, half] if par == 0 else halo_odd[i]
            column(src, cor_recv[par, i, 0, half], cor_recv[par, i, 1, half], buf.at[half, (cols + 1) * (1 - sx)], scale, shift)

    def run_layer(par, first, pair_of, weights, bias, skip, residual, last, after):
        halves = 2 if first else 1

        await_copies(par, first, 0, True)
        start = norms(par, first, 0, pair_of)
        halo_column(par, first, 0, act_a, start)

        def own(c, _):
            for half, (scale, shift) in enumerate(start):
                own_column(par, 0, half, c, act_a.at[half, c + 1], scale, shift)
            return 0

        lax.fori_loop(0, cols, own, 0)

        def step(i, s):
            now, later = acts[s], acts[1 - s]
            if s == 0:
                ahead = i + 1
                await_copies(par, first, ahead, False)
            else:
                ahead = jnp.minimum(i + 1, samples - 1)

                @pl.when(i + 1 < samples)
                def _():
                    await_copies(par, first, ahead, False)

            factors = norms(par, first, ahead, pair_of)

            def quad(t, sums):
                rows_of = []
                for q in range(2):
                    p = 2 * t + q
                    pieces = []
                    for dr in range(3):
                        for j in range(4):
                            for half in range(halves):
                                pieces.append(now[half, 2 * p + j, dr:dr + segrows].reshape(px, LANES))
                    if skip:
                        for e in range(2):
                            for half in range(2):
                                pieces.append(wide[i, half, 2 * p + e].reshape(px, LANES))
                    rows_of.append(jnp.concatenate(pieces, axis=1))
                res = jnp.dot(jnp.concatenate(rows_of, axis=0), weights(), preferred_element_type=F32)
                for half, (scale, shift) in enumerate(factors):
                    for e in range(4):
                        own_column(par, ahead, half, 4 * t + e, later.at[half, 4 * t + e + 1], scale, shift)
                s_one, s_two = sums
                for q in range(2):
                    for e in range(2):
                        c = 4 * t + 2 * q + e
                        y = res[q * px:(q + 1) * px, e * LANES:(e + 1) * LANES] + bias
                        if residual:
                            y = y + wide[i, 0, c].reshape(px, LANES).astype(F32)
                        rounded = y.astype(BF16)
                        if par == 0:
                            thin[i, c] = rounded.reshape(segrows, SEGS, LANES)
                        else:
                            wide[i, 0, c] = rounded.reshape(segrows, SEGS, LANES)
                        back = rounded.astype(F32).reshape(px // 8, 8, LANES)
                        s_one = s_one + jnp.sum(back, axis=0)
                        s_two = s_two + jnp.sum(back * back, axis=0)
                return s_one, s_two

            zero = jnp.zeros((8, LANES), F32)
            sums = lax.fori_loop(0, cols // 4, quad, (zero, zero))
            send(1 - par, False, i, [sums], False)
            if not last:
                @pl.when(i >= DEFER)
                def _():
                    column_copy(1 - par, False, i - DEFER).start()

            if not first:
                @pl.when(i < DEFER)
                def _():
                    column_copy(par, False, i + samples - DEFER).start()

            after(i)
            if s == 0:
                column_copy(par, first, ahead).wait()
                halo_column(par, first, ahead, later, factors)
            else:
                @pl.when(i + 1 < samples)
                def _():
                    column_copy(par, first, ahead).wait()
                    halo_column(par, first, ahead, later, factors)

        def two(t, _):
            step(2 * t, 0)
            step(2 * t + 1, 1)
            return 0

        lax.fori_loop(0, samples // 2, two, 0)

    def rest_pair(at):
        def pair_of(half):
            pair = nr_ref[at].astype(F32)
            return pair[0:1], pair[1:2]
        return pair_of

    def first_pair(half):
        pair = nf_ref[:, half * LANES:(half + 1) * LANES].astype(F32)
        return pair[0:1], pair[1:2]

    def edge_copy(i):
        return pltpu.make_async_remote_copy(
            src_ref=q_send.at[i], dst_ref=q_recv.at[i], send_sem=q_ss.at[i], recv_sem=q_rs.at[i],
            device_id={"sx": 1 - sx, "sy": sy}, device_id_type=MESH)

    def head_products(i):
        await_copies(0, False, i, False)
        (scale, shift), = norms(0, False, i, rest_pair(5))
        buf = act_b.at[1]
        prods = []
        for c in range(0, cols, 2):
            for e in range(2):
                own_column(0, i, 0, c + e, buf.at[c + e + 1], scale, shift)
            both = jnp.concatenate([buf[c + e + 1].reshape(px + 2 * SEGS, LANES) for e in range(2)], axis=1)
            prods.append(lax.dot_general(head_w[...], both, (((1,), (1,)), ((), ())), preferred_element_type=F32))

        def tap(c, dr, kc):
            at = 72 * (c % 2) + 24 * dr + 8 * kc
            return prods[c // 2][at:at + 8]

        def shifted(taps):
            return sum(taps[dr][:, dr * SEGS:dr * SEGS + px] for dr in range(3))

        q_send[i] = shifted([jnp.where(sx == 0, tap(cols - 1, dr, 0), tap(0, dr, 2)) for dr in range(3)])[0:4]
        edge_copy(i).start()
        slot = lax.rem(i, 4)
        for c in range(cols):
            near = [kc for kc in range(3) if 0 <= c + kc - 1 < cols]
            y = shifted([sum(tap(c + kc - 1, dr, kc) for kc in near) for dr in range(3)])
            for ch in range(3):
                image[slot, ch * cols + c:ch * cols + c + 1, :] = y[ch:ch + 1]

    def head_finish(i):
        edge_copy(i).wait()
        slot = lax.rem(i, 4)
        for ch in range(3):
            at = pl.ds(ch * cols + edge, 1)
            image[slot, at, :] = image[slot, at, :] + q_recv[i][ch:ch + 1]
        y = image[slot]
        high = y.astype(BF16).astype(F32)
        rest = y - high
        mid = rest.astype(BF16).astype(F32)
        split = jnp.concatenate([high, mid, rest - mid], axis=0).astype(BF16)
        moved = jnp.dot(split, order[...], preferred_element_type=F32)
        n = 3 * cols
        moved = moved[0:n] + (moved[n:2 * n] + moved[2 * n:3 * n])
        shift = bo_ref[...].astype(F32)
        for ch in range(3):
            out_ref[i, ch] = moved[ch * cols:(ch + 1) * cols] + shift[0:1, ch:ch + 1]

    def nothing(i):
        pass

    def head(i):
        @pl.when(i >= HEAD_LAG)
        def _():
            head_products(i - HEAD_LAG)

        @pl.when(i >= EDGE_LAG)
        def _():
            head_finish(i - EDGE_LAG)

    run_layer(0, True, first_pair, lambda: w_one[...].reshape(24 * LANES, 2 * LANES), bias_f[0:1], False, False, False, nothing)
    run_layer(1, False, rest_pair(0), lambda: w_two[...].reshape(16 * LANES, 2 * LANES), bias_f[1:2] + bias_f[6:7], True, False, False, nothing)
    for at in range(4):
        weights = functools.partial(lambda n: w_mid[n].reshape(12 * LANES, 2 * LANES), at)
        run_layer(at % 2, False, rest_pair(at + 1), weights, bias_f[at + 2:at + 3], False, at % 2 == 1, at == 3, head if at == 3 else nothing)

    def tail(i, _):
        @pl.when(i < samples + HEAD_LAG)
        def _():
            head_products(i - HEAD_LAG)

        head_finish(i - EDGE_LAG)
        return 0

    lax.fori_loop(samples, samples + EDGE_LAG, tail, 0)


def solution(mesh):
    n_sy = mesh.shape["sy"]
    n_sx = mesh.shape["sx"]
    devices = n_sx * n_sy
    tile_spec = P("dp", "sy", "sx", None)
    replicated = P()

    def local_decode(act_in, norm_first, w_first, w_short, norm_rest, w_rest, bias_rest, w_out, bias_out):
        samples, rows, cols, chans = act_in.shape
        segrows = rows // SEGS
        act_five = act_in.reshape(samples, SEGS, segrows, cols, chans)
        w_head = jnp.transpose(w_out, (0, 1, 3, 2))
        vmem = pl.BlockSpec(memory_space=pltpu.VMEM)
        hbm = pl.BlockSpec(memory_space=pl.ANY)
        dma = pltpu.SemaphoreType.DMA
        scratch = [
            pltpu.VMEM((samples, 2, cols, segrows, SEGS, LANES), BF16),
            pltpu.VMEM((samples, cols, segrows, SEGS, LANES), BF16),
            pltpu.VMEM((2, cols + 2, segrows + 2, SEGS, LANES), BF16),
            pltpu.VMEM((2, cols + 2, segrows + 2, SEGS, LANES), BF16),
            pltpu.VMEM((3, 4, 2 * LANES, 2 * LANES), BF16),
            pltpu.VMEM((4, 4, LANES, 2 * LANES), BF16),
            pltpu.VMEM((4, 3, 4, LANES, 2 * LANES), BF16),
            pltpu.VMEM((samples, 2, segrows, SEGS, LANES), BF16),
            pltpu.VMEM((samples, segrows, SEGS, LANES), BF16),
            pltpu.VMEM((2, SEGS, segrows, cols, chans), BF16),
            pltpu.VMEM((2, SEGS * cols, LANES), F32),
            pltpu.VMEM((7, LANES), F32),
            pltpu.VMEM((samples, 2, 2, cols, LANES), F32),
            pltpu.VMEM((2, samples, 2, 2, cols, LANES), F32),
            pltpu.VMEM((samples, 2, 2, 1, LANES), F32),
            pltpu.VMEM((2, samples, 2, 2, 1, LANES), F32),
            pltpu.VMEM((2, samples, devices, 2, 2, LANES), F32),
            pltpu.VMEM((2, 2 * (devices - 1) + 2 * cols + 2, LANES), F32),
            pltpu.VMEM((144, 2 * LANES), F32),
            pltpu.VMEM((144, 2 * LANES), BF16),
            pltpu.VMEM((segrows * SEGS, segrows * SEGS), BF16),
            pltpu.VMEM((4, 3 * cols, segrows * SEGS), F32),
            pltpu.VMEM((samples, 4, segrows * SEGS), F32),
            pltpu.VMEM((samples, 4, segrows * SEGS), F32),
            dma((2,)),
            dma((40,)),
            dma((2, samples)),
            dma((2, samples)),
            dma((2, samples)),
            dma((2, samples)),
            dma((samples,)),
            dma((samples,)),
        ]
        cfg = (samples, segrows, cols, n_sx, n_sy)
        image = pl.pallas_call(
            functools.partial(decode_kernel, cfg),
            out_shape=jax.ShapeDtypeStruct((samples, 3, cols, rows), F32),
            in_specs=[hbm, vmem, hbm, hbm, vmem, hbm, vmem, vmem, vmem],
            out_specs=vmem,
            scratch_shapes=scratch,
            compiler_params=pltpu.CompilerParams(collective_id=0, has_side_effects=True, vmem_limit_bytes=67043328),
        )(act_five, norm_first, w_first, w_short, norm_rest, w_rest, bias_rest, w_head, bias_out.reshape(1, 3))
        return jnp.transpose(image, (0, 3, 2, 1))

    return jax.shard_map(local_decode, mesh=mesh, in_specs=(tile_spec, replicated, replicated, replicated, replicated, replicated, replicated, replicated, replicated), out_specs=tile_spec, check_vma=False)
```
